256 devices in a mesh: seq: 64 (over z, x, core), head: 4 (over y).
Axes of the slice: x: 4, y: 4, z: 8, core: 2. Of those that a mesh axis runs over, the one named last changes fastest.
Arguments:
- query: bfloat16 [32768, 4096], P(('seq', 'head')), may hold values from -6 to 6
- key: bfloat16 [32768, 1024], P(('seq', 'head')), may hold values from -6 to 6
- value: bfloat16 [32768, 1024], P(('seq', 'head')), may hold values from -6 to 6
- out: bfloat16 [32768, 4096], P(('seq', 'head')), may hold values from -4 to 4
- output_gradient: bfloat16 [32768, 4096], P(('seq', 'head')), may hold values from -6 to 6
- log_sum_exp: float32 [32768, 32], P(('seq', 'head')), may hold values from 4 to 7
- segment_ids: int32 [32768], replicated, may hold values from 0 to 31, never falling along the last dimension, each value on 1 to 1536 neighbouring positions
Outputs:
- d_query: bfloat16 [32768, 4096], P(('seq', 'head'))
- key_gradient: bfloat16 [32768, 1024], P(('seq', 'head'))
- value_gradient: bfloat16 [32768, 1024], P(('seq', 'head'))
The draws below stay inside these ranges and needn't reach their ends.
Inputs may be any that keep to these rules, and one draw needn't show every extreme that they name: `segment_ids`: never falls along the positions; a document holds at most 1536 positions, and one holds exactly 1536.
All inputs are finite; a program needn't handle non-finite values.
Results may differ from the reference program's by a relative error of at most 0.0071.
Values may be sent and summed in bfloat16 or wider, within the bound.
A program may use at most 128 MiB of HBM per device.

```python
import math
import jax
import jax.numpy as jnp
import numpy as np
from jax import lax

QUERY_HEADS = 32
KEY_VALUE_HEADS = 8
HEAD_SIZE = 128
TOK_DEV = 128
REACH = 3
PACKED_TOKENS = 32768
MOST = 1536
DOCS = 32
N_HEAD = 4


def block_levels(rng, shape, pieces, low, top_value):
    level, own = 1.0, jax.random.fold_in(rng, 6)
    for axis_at, shards_of in pieces:
        heights = jnp.exp(jax.random.uniform(jax.random.fold_in(own, axis_at), (shards_of,), jnp.float32, low / len(pieces), top_value / len(pieces)))
        level = level * jnp.repeat(heights, shape[axis_at] // shards_of).reshape([-1 if axis == axis_at else 1 for axis in range(len(shape))])
    return level


def split_up(number_of, total, most, slope):
    portions = [(1 << 20) // math.isqrt(rank ** slope) + 1 for rank in range(2, number_of + 1)]
    spare, counts = total - most - (number_of - 1), [1] * (number_of - 1)
    while spare > 0:
        movable = [i for i in range(number_of - 1) if counts[i] < most]
        pool, budget = sum([portions[i] for i in movable]), spare
        for i in movable:
            more = min(most - counts[i], max(1, budget * portions[i] // pool), spare)
            counts[i] = counts[i] + more
            spare = spare - more
    return np.array([most] + counts)


def uneven_parts(key, number_of, total, most, lean):
    if number_of == 2:
        one = jax.random.randint(key, (), max(1, total - most), min(most, total - 1) + 1)
        return jnp.stack([one, total - one])
    sizes = jnp.asarray(split_up(number_of, total, most, lean), jnp.int32)
    couples = (number_of - 1) // 2
    donor, sink = sizes[1:1 + 2 * couples:2], sizes[2:2 + 2 * couples:2]
    slack = jnp.minimum(donor - 1, most - sink)
    moved = jax.random.randint(jax.random.fold_in(key, 1), (couples,), 0, 1 << 20) % (slack + 1)
    sizes = sizes.at[1:1 + 2 * couples:2].set(donor - moved).at[2:2 + 2 * couples:2].set(sink + moved)
    return sizes[jax.random.permutation(jax.random.fold_in(key, 2), number_of)]


def noise(rng, shape, width, bound, cuts=(), kind=jnp.bfloat16):
    level = block_levels(rng, shape, cuts, -0.22, 0.18) if cuts else 1.0
    entries = jax.random.normal(rng, shape, jnp.float32) * width * level
    return jnp.minimum(jnp.maximum(entries, -bound), bound).astype(kind)


def setup_inputs(seed: int = 0) -> dict:
    streams_of = jax.random.split(jax.random.key(seed), 8)
    query = noise(streams_of[0], (PACKED_TOKENS, QUERY_HEADS * HEAD_SIZE), 1.0, 6.0, ((0, 256),))
    key = noise(streams_of[1], (PACKED_TOKENS, KEY_VALUE_HEADS * HEAD_SIZE), 1.0, 6.0, ((0, 256),))
    value = noise(streams_of[2], (PACKED_TOKENS, KEY_VALUE_HEADS * HEAD_SIZE), 1.0, 6.0, ((0, 256),))
    out = noise(streams_of[3], (PACKED_TOKENS, QUERY_HEADS * HEAD_SIZE), 0.5, 4.0, ((0, 256),))
    output_gradient = noise(streams_of[4], (PACKED_TOKENS, QUERY_HEADS * HEAD_SIZE), 1.0, 6.0, ((0, 256),))
    log_sum_exp = jnp.clip(4.0 + 3.0 * jax.random.uniform(streams_of[5], (PACKED_TOKENS, QUERY_HEADS), jnp.float32) ** block_levels(streams_of[5], (PACKED_TOKENS, QUERY_HEADS), ((0, 256),), -0.2, 0.2), 4.0, 7.0)
    segment_ids = jnp.searchsorted(jnp.cumsum(uneven_parts(streams_of[6], DOCS, PACKED_TOKENS, MOST, 2)), jnp.arange(PACKED_TOKENS), side="right").astype(jnp.int32)
    return {"query": query, "key": key, "value": value, "out": out, "output_gradient": output_gradient, "log_sum_exp": log_sum_exp, "segment_ids": segment_ids}


def rounded(values):
    return lax.optimization_barrier(values.astype(jnp.bfloat16)).astype(jnp.float32)

def reference(query, key, value, out, output_gradient, log_sum_exp, segment_ids):
    row_number = TOK_DEV * N_HEAD
    block_list = PACKED_TOKENS // row_number
    group_width = QUERY_HEADS // KEY_VALUE_HEADS
    score_scale = 1.0 / math.sqrt(HEAD_SIZE)
    padding_rows = REACH * row_number
    window_rows = (REACH + 1) * row_number
    query_total = query.astype(jnp.float32).reshape(block_list, row_number, KEY_VALUE_HEADS, group_width, HEAD_SIZE)
    gradient_total = output_gradient.astype(jnp.float32).reshape(block_list, row_number, KEY_VALUE_HEADS, group_width, HEAD_SIZE)
    output_total = out.astype(jnp.float32).reshape(block_list, row_number, KEY_VALUE_HEADS, group_width, HEAD_SIZE)
    delta_all = lax.optimization_barrier(jnp.sum(gradient_total * output_total, axis=4))
    log_sum_exp_total = log_sum_exp.astype(jnp.float32).reshape(block_list, row_number, KEY_VALUE_HEADS, group_width)
    key_padded = jnp.concatenate([jnp.zeros((padding_rows, KEY_VALUE_HEADS * HEAD_SIZE), jnp.float32), key.astype(jnp.float32)], axis=0).reshape(padding_rows + PACKED_TOKENS, KEY_VALUE_HEADS, HEAD_SIZE)
    value_padded = jnp.concatenate([jnp.zeros((padding_rows, KEY_VALUE_HEADS * HEAD_SIZE), jnp.float32), value.astype(jnp.float32)], axis=0).reshape(padding_rows + PACKED_TOKENS, KEY_VALUE_HEADS, HEAD_SIZE)
    seg_ids = segment_ids.astype(jnp.int32)
    seg_pad = jnp.concatenate([jnp.full((padding_rows,), -1, jnp.int32), seg_ids])
    query_offsets = jnp.arange(row_number, dtype=jnp.int32) + padding_rows
    key_offsets = jnp.arange(window_rows, dtype=jnp.int32)

    def block_step(accums, inputs):
        key_gradient_total, value_gradient_total = accums
        query_heads, grad_heads, delta_rows, lse_rows, index = inputs
        window_start = (index * row_number).astype(jnp.int32)
        key_block = lax.dynamic_slice_in_dim(key_padded, window_start, window_rows, 0)
        value_block = lax.dynamic_slice_in_dim(value_padded, window_start, window_rows, 0)
        seg_keys = lax.dynamic_slice_in_dim(seg_pad, window_start, window_rows, 0)
        seg_query = lax.dynamic_slice_in_dim(seg_ids, window_start, row_number, 0)
        allowed = (seg_query[:, None] == seg_keys[None, :]) & (key_offsets[None, :] <= query_offsets[:, None])
        lse_cols = lse_rows.transpose(1, 2, 0)[..., None]
        delta_cols = delta_rows.transpose(1, 2, 0)[..., None]
        scores = jnp.einsum('igmd,jgd->gmij', query_heads, key_block) * score_scale
        probs = jnp.exp(jnp.where(allowed, scores - lse_cols, -jnp.inf))
        probs_low = rounded(probs)
        dprobs = jnp.einsum('igmd,jgd->gmij', grad_heads, value_block)
        dscores = rounded(score_scale * probs * (dprobs - delta_cols))
        grad_query = jnp.einsum('gmij,jgd->igmd', dscores, key_block)
        grad_key = jnp.einsum('gmij,igmd->jgd', dscores, query_heads)
        grad_value = jnp.einsum('gmij,igmd->jgd', probs_low, grad_heads)
        key_gradient_total = lax.dynamic_update_slice_in_dim(key_gradient_total, lax.dynamic_slice_in_dim(key_gradient_total, window_start, window_rows, 0) + grad_key, window_start, 0)
        value_gradient_total = lax.dynamic_update_slice_in_dim(value_gradient_total, lax.dynamic_slice_in_dim(value_gradient_total, window_start, window_rows, 0) + grad_value, window_start, 0)
        return ((key_gradient_total, value_gradient_total), grad_query.astype(jnp.bfloat16))
    starting_totals = (jnp.zeros((padding_rows + PACKED_TOKENS, KEY_VALUE_HEADS, HEAD_SIZE), jnp.float32), jnp.zeros((padding_rows + PACKED_TOKENS, KEY_VALUE_HEADS, HEAD_SIZE), jnp.float32))
    indices = jnp.arange(block_list, dtype=jnp.int32)
    (key_gradient_total, value_gradient_total), grad_blocks = lax.scan(block_step, starting_totals, (query_total, gradient_total, delta_all, log_sum_exp_total, indices))
    d_query = grad_blocks.reshape(PACKED_TOKENS, QUERY_HEADS * HEAD_SIZE)
    key_gradient = key_gradient_total[padding_rows:].reshape(PACKED_TOKENS, KEY_VALUE_HEADS * HEAD_SIZE).astype(jnp.bfloat16)
    value_gradient = value_gradient_total[padding_rows:].reshape(PACKED_TOKENS, KEY_VALUE_HEADS * HEAD_SIZE).astype(jnp.bfloat16)
    return (d_query, key_gradient, value_gradient)
```

```python
import functools
import math

import jax
import jax.numpy as jnp
from jax import lax
from jax.experimental import pallas as pl
from jax.experimental.pallas import tpu as pltpu
from jax.sharding import PartitionSpec as P

MESH = pl.DeviceIdType.MESH
BF16 = jnp.bfloat16
F32 = jnp.float32

HEAD = 128
TOK = 128
GROUP = 4
Y = 4
PIECES = 8
SPAN = PIECES * TOK
HALF = SPAN // 2
HALO = SPAN + HALF
BLOCK = 256
HALO_BLOCKS = HALO // BLOCK
SPAN_BLOCKS = SPAN // BLOCK
QCOLS = GROUP * HEAD

LOG2E = math.log2(math.e)
SCALE = 1.0 / math.sqrt(HEAD)
SHIFT = 4.0
REST = SCALE * 2.0**SHIFT
NT = (((1,), (1,)), ((), ()))
TN = (((0,), (0,)), ((), ()))


def kernel(
    n_span,
    q_hbm, k_hbm, v_hbm, o_hbm, e_hbm, lse_ref, seg_ref,
    dq_out, dk_out, dv_out,
    k_src, v_src, o_src, e_src, aux_src,
    k_all, v_all, q_all, e_all, aux, seg_k, seg_q,
    dq_t, dk_acc, dv_acc,
    dq_send, dk_send, dv_send, dk_back, dv_back, dk_near, dv_near, dk_far, dv_far,
    load_sem, kv_send, kv_recv, aux_send, aux_recv, qe_send, qe_recv,
    halo_send, halo_recv, back_send, back_recv, out_send, out_recv,
):
    seq = lax.axis_index("seq")
    y = lax.axis_index("head")
    span = lax.div(seq, 2)
    core = lax.rem(seq, 2)
    mine = core * Y + y
    group = y * 2 + core

    def piece_device(piece):
        return (span * 2 + piece // Y, piece % Y)

    def span_device(by):
        return (seq + 2 * by, y)

    peers = []
    for dy in (1, 3, 2, 0):
        for dcore in (0, 1):
            if dy or dcore:
                py = lax.rem(y + dy, Y)
                pcore = lax.rem(core + dcore, 2)
                peers.append((dy * 2 + dcore, (span * 2 + pcore, py), py * 2 + pcore))

    has_prev, has_prev2 = span >= 1, span >= 2
    has_next, has_next2 = span < n_span - 1, span < n_span - 2

    def cols(g, width):
        return pl.ds(pl.multiple_of(g * width, width), width)

    my_rows = pl.ds(pl.multiple_of(mine * TOK, TOK), TOK)
    my_key_rows = pl.ds(pl.multiple_of(HALO + mine * TOK, TOK), TOK)
    loads = [
        pltpu.make_async_copy(src, dst, load_sem.at[i])
        for i, (src, dst) in enumerate(
            ((k_hbm, k_src), (v_hbm, v_src), (e_hbm, e_src), (o_hbm, o_src))
        )
    ]
    own = [
        pltpu.make_async_copy(k_hbm.at[:, cols(group, HEAD)], k_all.at[my_key_rows, :], kv_recv.at[0, mine]),
        pltpu.make_async_copy(v_hbm.at[:, cols(group, HEAD)], v_all.at[my_key_rows, :], kv_recv.at[1, mine]),
    ]
    for h in range(GROUP):
        columns = pl.ds(pl.multiple_of(group * QCOLS + h * HEAD, HEAD), HEAD)
        for i, (src, dst) in enumerate(((q_hbm, q_all), (e_hbm, e_all))):
            own.append(
                pltpu.make_async_copy(
                    src.at[:, columns], dst.at[my_rows, pl.ds(h * HEAD, HEAD)], qe_recv.at[i, h, mine]
                )
            )
    for copy in loads + own:
        copy.start()

    barrier = pltpu.get_barrier_semaphore()

    def greet(device):
        pl.semaphore_signal(barrier, inc=1, device_id=device, device_id_type=MESH)

    for _, device, _ in peers:
        greet(device)
    pl.when(has_prev)(lambda: greet(span_device(-1)))
    pl.when(has_prev2)(lambda: greet(span_device(-2)))
    pl.when(has_next)(lambda: greet(span_device(1)))
    pl.when(has_next2)(lambda: greet(span_device(2)))
    neighbours = jnp.minimum(span, 2) + jnp.minimum(n_span - 1 - span, 2)
    pl.semaphore_wait(barrier, len(peers) + neighbours)

    def remote(src, dst, send, recv, device):
        return pltpu.make_async_remote_copy(
            src_ref=src, dst_ref=dst, send_sem=send, recv_sem=recv, device_id=device, device_id_type=MESH
        )

    sends = []
    loads[0].wait()
    loads[1].wait()
    for n, device, g in peers:
        for i, (src, dst) in enumerate(((k_src, k_all), (v_src, v_all))):
            sends.append(
                remote(src.at[:, cols(g, HEAD)], dst.at[my_key_rows, :], kv_send.at[i, n], kv_recv.at[i, mine], device)
            )
            sends[-1].start()

    loads[2].wait()
    for h in range(GROUP):
        for n, device, g in peers:
            columns = pl.ds(pl.multiple_of(g * QCOLS + h * HEAD, HEAD), HEAD)
            for i, (src, dst) in enumerate(((q_hbm, q_all), (e_src, e_all))):
                sends.append(
                    remote(
                        src.at[:, columns], dst.at[my_rows, pl.ds(h * HEAD, HEAD)],
                        qe_send.at[i, h, n], qe_recv.at[i, h, mine], device,
                    )
                )
                sends[-1].start()
        if h == 0:
            loads[3].wait()
            lane = lax.broadcasted_iota(jnp.int32, (TOK, HEAD), 1)
            delta = jnp.zeros((TOK, HEAD), F32)
            for head in range(PIECES * GROUP):
                part = pl.ds(head * HEAD, HEAD)
                product = e_src[:, part].astype(F32) * o_src[:, part].astype(F32)
                delta = jnp.where(lane == head, jnp.sum(product, axis=1, keepdims=True), delta)
            delta = delta.T
            lse = jnp.concatenate([lse_ref[...], jnp.zeros((TOK, HEAD - PIECES * GROUP), F32)], axis=1).T
            lse = lse * LOG2E + SHIFT
            for g in range(PIECES):
                aux_src[g, 0:GROUP, :] = lse[g * GROUP : (g + 1) * GROUP, :]
                aux_src[g, GROUP : 2 * GROUP, :] = delta[g * GROUP : (g + 1) * GROUP, :]
            for n, device, g in peers:
                sends.append(remote(aux_src.at[g], aux.at[mine], aux_send.at[n], aux_recv.at[mine], device))
                sends[-1].start()
            aux[mine] = aux_src[group]

    first = span * PIECES - HALO // TOK
    for i in range((HALO + SPAN) // TOK):
        row = seg_ref[pl.ds(jnp.maximum(first + i, 0), 1), :]
        row = jnp.where(first + i < 0, -1, row)
        seg_k[pl.ds(i * TOK, TOK), :] = jnp.broadcast_to(row, (TOK, TOK)).T
        if i >= HALO // TOK:
            seg_q[:, pl.ds(i * TOK - HALO, TOK)] = row

    dk_acc[...] = jnp.zeros_like(dk_acc)
    dv_acc[...] = jnp.zeros_like(dv_acc)
    dq_t[...] = jnp.zeros_like(dq_t)

    def halo_copies(by, piece):
        rows = pl.ds(HALO + piece * TOK, TOK)
        to = pl.ds((HALF if by == 1 else -HALF) + piece * TOK, TOK)
        at = piece if by == 1 else piece + Y
        return [
            remote(ref.at[rows, :], ref.at[to, :], halo_send.at[i, at], halo_recv.at[i, at], span_device(by))
            for i, ref in enumerate((k_all, v_all))
        ]

    def start_all(copies):
        for copy in copies:
            copy.start()

    def here(ref, sem):
        return pltpu.make_async_copy(ref, ref, sem)

    for piece in reversed(range(PIECES)):
        rows = pl.ds(HALO + piece * TOK, TOK)
        here(k_all.at[rows, :], kv_recv.at[0, piece]).wait()
        here(v_all.at[rows, :], kv_recv.at[1, piece]).wait()
        pl.when(has_next)(lambda: start_all(halo_copies(1, piece)))
        if piece >= Y:
            pl.when(has_next2)(lambda: start_all(halo_copies(2, piece)))

    for piece in range(PIECES):
        pl.when(mine != piece)(lambda: here(aux.at[piece], aux_recv.at[piece]).wait())

    def step(j, h, r0, r1):
        keys = pl.ds(j * BLOCK, BLOCK)
        width = (r1 - r0) * BLOCK
        rows = pl.ds(r0 * BLOCK, width)
        columns = pl.ds(pl.multiple_of(h * HEAD, HEAD), HEAD)
        q, e = q_all[rows, columns], e_all[rows, columns]
        k, v = k_all[keys, :], v_all[keys, :]
        scores = lax.dot_general(k, q, NT, preferred_element_type=F32)
        dprobs = lax.dot_general(v, e, NT, preferred_element_type=F32)
        pieces = range(r0 * BLOCK // TOK, r1 * BLOCK // TOK)
        lse = jnp.concatenate([aux[p, pl.ds(h, 1), :] for p in pieces], axis=1)
        delta = jnp.concatenate([aux[p, pl.ds(h + GROUP, 1), :] for p in pieces], axis=1)
        doc = jnp.concatenate([seg_k[keys, :]] * (width // TOK), axis=1)
        allowed = doc == seg_q[:, rows]
        if j >= HALO_BLOCKS:
            key_at = lax.broadcasted_iota(jnp.int32, (BLOCK, width), 0) + (j - HALO_BLOCKS) * BLOCK
            query_at = lax.broadcasted_iota(jnp.int32, (BLOCK, width), 1) + r0 * BLOCK
            allowed = allowed & (key_at <= query_at)
        probs = jnp.exp2(jnp.where(allowed, scores * (SCALE * LOG2E) - lse, -jnp.inf))
        dscores = (probs * (dprobs - delta)).astype(BF16)
        probs = probs.astype(BF16)
        dv_acc[keys, :] += jnp.dot(probs, e, preferred_element_type=F32)
        dk_acc[keys, :] += jnp.dot(dscores, q, preferred_element_type=F32)
        dq_t[h, :, rows] += lax.dot_general(k, dscores, TN, preferred_element_type=F32)

    def own_head(h, carry):
        for piece in range(PIECES):
            rows = pl.ds(piece * TOK, TOK)
            columns = pl.ds(pl.multiple_of(h * HEAD, HEAD), HEAD)
            here(q_all.at[rows, columns], qe_recv.at[0, h, piece]).wait()
            here(e_all.at[rows, columns], qe_recv.at[1, h, piece]).wait()
        for b in range(SPAN_BLOCKS):
            step(HALO_BLOCKS + b, h, b, SPAN_BLOCKS)
        return carry

    lax.fori_loop(0, GROUP, own_head, 0)

    def dq_copy(piece):
        return remote(
            dq_send.at[pl.ds(piece * TOK, TOK), :], dq_out.at[:, cols(group, QCOLS)],
            out_send.at[0, piece], out_recv.at[0, group], piece_device(piece),
        )

    def dq_local(piece):
        return pltpu.make_async_copy(
            dq_send.at[pl.ds(piece * TOK, TOK), :], dq_out.at[:, cols(group, QCOLS)], out_recv.at[0, group]
        )

    def finish_rows(r):
        rows = pl.ds(r * BLOCK, BLOCK)
        for h in range(GROUP):
            dq_send[rows, pl.ds(h * HEAD, HEAD)] = (dq_t[h, :, rows].T * REST).astype(BF16)
        for piece in (2 * r, 2 * r + 1):
            pl.when(mine != piece)(lambda: dq_copy(piece).start())
            pl.when(mine == piece)(lambda: dq_local(piece).start())

    def back_copies(j):
        rows = pl.ds(j * BLOCK, BLOCK)
        if j * BLOCK >= HALF:
            dsts, at, by = (dk_near, dv_near), pl.ds(j * BLOCK - HALF, BLOCK), -1
        else:
            dsts, at, by = (dk_far, dv_far), rows, -2
        return [
            remote(src.at[rows, :], dst.at[at, :], back_send.at[i, j], back_recv.at[i, j], span_device(by))
            for i, (src, dst) in enumerate(((dk_back, dsts[0]), (dv_back, dsts[1])))
        ]

    def halo_block(j):
        rows = pl.ds(j * BLOCK, BLOCK)
        far = j * BLOCK < HALF
        for piece in (2 * j, 2 * j + 1):
            at = (piece + PIECES) if far else piece - Y
            at_rows = pl.ds(piece * TOK, TOK)
            here(k_all.at[at_rows, :], halo_recv.at[0, at]).wait()
            here(v_all.at[at_rows, :], halo_recv.at[1, at]).wait()

        def head(h, carry):
            step(j, h, max(0, j - HALO_BLOCKS), min(SPAN_BLOCKS, j + 1))
            return carry

        lax.fori_loop(0, GROUP, head, 0)
        dk_back[rows, :] = (dk_acc[rows, :] * REST).astype(BF16)
        dv_back[rows, :] = (dv_acc[rows, :] * 2.0**SHIFT).astype(BF16)
        start_all(back_copies(j))

    for j in reversed(range(HALO_BLOCKS)):
        pl.when(has_prev if j * BLOCK >= HALF else has_prev2)(lambda: halo_block(j))
        if j < SPAN_BLOCKS:
            finish_rows(j)

    def dkv_copies(piece):
        rows = pl.ds(piece * TOK, TOK)
        return [
            remote(
                src.at[rows, :], dst.at[:, cols(group, HEAD)],
                out_send.at[i, piece], out_recv.at[i, group], piece_device(piece),
            )
            for i, src, dst in ((1, dk_send, dk_out), (2, dv_send, dv_out))
        ]

    def dkv_local(piece):
        rows = pl.ds(piece * TOK, TOK)
        return [
            pltpu.make_async_copy(src.at[rows, :], dst.at[:, cols(group, HEAD)], out_recv.at[i, group])
            for i, src, dst in ((1, dk_send, dk_out), (2, dv_send, dv_out))
        ]

    def finish_keys(b):
        rows = pl.ds(b * BLOCK, BLOCK)
        acc_rows = pl.ds(HALO + b * BLOCK, BLOCK)
        for i, acc, near, far, out, factor in (
            (0, dk_acc, dk_near, dk_far, dk_send, REST),
            (1, dv_acc, dv_near, dv_far, dv_send, 2.0**SHIFT),
        ):
            acc[acc_rows, :] *= factor

            def add_near():
                here(near.at[rows, :], back_recv.at[i, b + HALF // BLOCK]).wait()
                acc[acc_rows, :] += near[rows, :].astype(F32)

            def add_far():
                far_rows = pl.ds(b * BLOCK - HALF, BLOCK)
                here(far.at[far_rows, :], back_recv.at[i, b - HALF // BLOCK]).wait()
                acc[acc_rows, :] += far[far_rows, :].astype(F32)

            pl.when(has_next)(add_near)
            if b * BLOCK >= HALF:
                pl.when(has_next2)(add_far)
            out[rows, :] = acc[acc_rows, :].astype(BF16)
        for piece in (2 * b, 2 * b + 1):
            pl.when(mine != piece)(lambda: start_all(dkv_copies(piece)))
            pl.when(mine == piece)(lambda: start_all(dkv_local(piece)))

    for b in (1, 0, 3, 2):
        finish_keys(b)

    for g in range(PIECES):
        here(dq_out.at[:, pl.ds(g * QCOLS, QCOLS)], out_recv.at[0, g]).wait()
        here(dk_out.at[:, pl.ds(g * HEAD, HEAD)], out_recv.at[1, g]).wait()
        here(dv_out.at[:, pl.ds(g * HEAD, HEAD)], out_recv.at[2, g]).wait()
    for copy in sends:
        copy.wait_send()

    def wait_sends(copies):
        for copy in copies:
            copy.wait_send()

    for piece in range(PIECES):
        pl.when(has_next)(lambda: wait_sends(halo_copies(1, piece)))
        if piece >= Y:
            pl.when(has_next2)(lambda: wait_sends(halo_copies(2, piece)))
        pl.when(mine != piece)(lambda: wait_sends([dq_copy(piece)] + dkv_copies(piece)))
    for j in range(HALO_BLOCKS):
        pl.when(has_prev if j * BLOCK >= HALF else has_prev2)(lambda: wait_sends(back_copies(j)))


def shards(n_span, query, key, value, out, output_gradient, log_sum_exp, segment_ids):
    any_space = pl.BlockSpec(memory_space=pl.ANY)
    vmem = pl.BlockSpec(memory_space=pltpu.VMEM)
    dma = pltpu.SemaphoreType.DMA
    shape = jax.ShapeDtypeStruct
    window = HALO + SPAN
    return pl.pallas_call(
        functools.partial(kernel, n_span),
        out_shape=[
            shape(query.shape, BF16),
            shape(key.shape, BF16),
            shape(value.shape, BF16),
        ],
        in_specs=[any_space] * 5 + [vmem] * 2,
        out_specs=[any_space] * 3,
        scratch_shapes=[
            pltpu.VMEM((TOK, PIECES * HEAD), BF16),
            pltpu.VMEM((TOK, PIECES * HEAD), BF16),
            pltpu.VMEM((TOK, PIECES * QCOLS), BF16),
            pltpu.VMEM((TOK, PIECES * QCOLS), BF16),
            pltpu.VMEM((PIECES, 2 * GROUP, TOK), F32),
            pltpu.VMEM((window, HEAD), BF16),
            pltpu.VMEM((window, HEAD), BF16),
            pltpu.VMEM((SPAN, QCOLS), BF16),
            pltpu.VMEM((SPAN, QCOLS), BF16),
            pltpu.VMEM((PIECES, 2 * GROUP, TOK), F32),
            pltpu.VMEM((window, TOK), jnp.int32),
            pltpu.VMEM((1, SPAN), jnp.int32),
            pltpu.VMEM((GROUP, HEAD, SPAN), F32),
            pltpu.VMEM((window, HEAD), F32),
            pltpu.VMEM((window, HEAD), F32),
            pltpu.VMEM((SPAN, QCOLS), BF16),
            pltpu.VMEM((SPAN, HEAD), BF16),
            pltpu.VMEM((SPAN, HEAD), BF16),
            pltpu.VMEM((HALO, HEAD), BF16),
            pltpu.VMEM((HALO, HEAD), BF16),
            pltpu.VMEM((SPAN, HEAD), BF16),
            pltpu.VMEM((SPAN, HEAD), BF16),
            pltpu.VMEM((HALF, HEAD), BF16),
            pltpu.VMEM((HALF, HEAD), BF16),
            dma((4,)),
            dma((2, PIECES)),
            dma((2, PIECES)),
            dma((PIECES,)),
            dma((PIECES,)),
            dma((2, GROUP, PIECES)),
            dma((2, GROUP, PIECES)),
            dma((2, PIECES + Y)),
            dma((2, PIECES + Y)),
            dma((2, HALO_BLOCKS)),
            dma((2, HALO_BLOCKS)),
            dma((3, PIECES)),
            dma((3, PIECES)),
        ],
        name="attention_backward",
        compiler_params=pltpu.CompilerParams(
            collective_id=0, has_side_effects=True, vmem_limit_bytes=48 * 2**20
        ),
    )(query, key, value, out, output_gradient, log_sum_exp, segment_ids.reshape(-1, TOK))


def solution(mesh):
    rows = P(("seq", "head"), None)
    return jax.shard_map(
        functools.partial(shards, mesh.shape["seq"] // 2),
        mesh=mesh,
        in_specs=(rows,) * 6 + (P(),),
        out_specs=(rows,) * 3,
        check_vma=False,
    )
```

```python
import functools
import math

import jax
import jax.numpy as jnp
from jax import lax
from jax.experimental import pallas as pl
from jax.experimental.pallas import tpu as pltpu
from jax.sharding import PartitionSpec as P

MESH = pl.DeviceIdType.MESH
BF16 = jnp.bfloat16
F32 = jnp.float32

HEAD = 128
TOK = 128
GROUP = 4
Y = 4
PIECES = 8
SPAN = PIECES * TOK
HALF = SPAN // 2
HALO = SPAN + HALF
BLOCK = 256
HALO_BLOCKS = HALO // BLOCK
SPAN_BLOCKS = SPAN // BLOCK
QCOLS = GROUP * HEAD

LOG2E = math.log2(math.e)
SCALE = 1.0 / math.sqrt(HEAD)
SHIFT = 4.0
REST = SCALE * 2.0**SHIFT
NT = (((1,), (1,)), ((), ()))
TN = (((0,), (0,)), ((), ()))


def kernel(
    n_span,
    q_hbm, k_hbm, v_hbm, o_hbm, e_hbm, lse_hbm, seg_hbm,
    dq_out, dk_out, dv_out,
    k_src, v_src, o_src, e_src, lse_ref, seg_ref, aux_src,
    k_all, v_all, q_all, e_all, aux, seg_k, seg_q,
    dq_t, dk_acc, dv_acc,
    dq_send, dk_send, dv_send, dk_back, dv_back, dk_near, dv_near, dk_far, dv_far,
    load_sem, kv_send, kv_recv, aux_send, aux_recv, qe_send, qe_recv,
    halo_send, halo_recv, back_send, back_recv,
    dq_send_sem, dq_recv_sem, dkv_send_sem, dkv_recv_sem,
):
    seq = lax.axis_index("seq")
    y = lax.axis_index("head")
    span = lax.div(seq, 2)
    core = lax.rem(seq, 2)
    mine = core * Y + y
    group = y * 2 + core

    def piece_device(piece):
        return (span * 2 + piece // Y, piece % Y)

    def span_device(by):
        return (seq + 2 * by, y)

    peers = []
    for dy in (1, 3, 2, 0):
        for dcore in (0, 1):
            if dy or dcore:
                py = lax.rem(y + dy, Y)
                pcore = lax.rem(core + dcore, 2)
                peers.append((dy * 2 + dcore, (span * 2 + pcore, py), py * 2 + pcore))

    has_prev, has_prev2 = span >= 1, span >= 2
    has_next, has_next2 = span < n_span - 1, span < n_span - 2

    def cols(g, width):
        return pl.ds(pl.multiple_of(g * width, width), width)

    my_rows = pl.ds(pl.multiple_of(mine * TOK, TOK), TOK)
    my_key_rows = pl.ds(pl.multiple_of(HALO + mine * TOK, TOK), TOK)
    loads = [
        pltpu.make_async_copy(src, dst, load_sem.at[i])
        for i, (src, dst) in enumerate(
            (
                (k_hbm, k_src), (v_hbm, v_src), (e_hbm, e_src), (o_hbm, o_src),
                (lse_hbm, lse_ref), (seg_hbm, seg_ref),
            )
        )
    ]
    own = [
        pltpu.make_async_copy(k_hbm.at[:, cols(group, HEAD)], k_all.at[my_key_rows, :], kv_recv.at[0, mine]),
        pltpu.make_async_copy(v_hbm.at[:, cols(group, HEAD)], v_all.at[my_key_rows, :], kv_recv.at[1, mine]),
    ]
    for h in range(GROUP):
        columns = pl.ds(pl.multiple_of(group * QCOLS + h * HEAD, HEAD), HEAD)
        for i, (src, dst) in enumerate(((q_hbm, q_all), (e_hbm, e_all))):
            own.append(
                pltpu.make_async_copy(
                    src.at[:, columns], dst.at[my_rows, pl.ds(h * HEAD, HEAD)], qe_recv.at[i, h, mine]
                )
            )
    for copy in loads + own:
        copy.start()

    barrier = pltpu.get_barrier_semaphore()

    def greet(device):
        pl.semaphore_signal(barrier, inc=1, device_id=device, device_id_type=MESH)

    for _, device, _ in peers:
        greet(device)
    pl.when(has_prev)(lambda: greet(span_device(-1)))
    pl.when(has_prev2)(lambda: greet(span_device(-2)))
    pl.when(has_next)(lambda: greet(span_device(1)))
    pl.when(has_next2)(lambda: greet(span_device(2)))
    neighbours = jnp.minimum(span, 2) + jnp.minimum(n_span - 1 - span, 2)
    pl.semaphore_wait(barrier, len(peers) + neighbours)

    def remote(src, dst, send, recv, device):
        return pltpu.make_async_remote_copy(
            src_ref=src, dst_ref=dst, send_sem=send, recv_sem=recv, device_id=device, device_id_type=MESH
        )

    sends = []
    loads[0].wait()
    loads[1].wait()
    for n, device, g in peers:
        for i, (src, dst) in enumerate(((k_src, k_all), (v_src, v_all))):
            sends.append(
                remote(src.at[:, cols(g, HEAD)], dst.at[my_key_rows, :], kv_send.at[i, n], kv_recv.at[i, mine], device)
            )
            sends[-1].start()

    loads[2].wait()
    for h in range(GROUP):
        for n, device, g in peers:
            columns = pl.ds(pl.multiple_of(g * QCOLS + h * HEAD, HEAD), HEAD)
            for i, (src, dst) in enumerate(((q_hbm, q_all), (e_src, e_all))):
                sends.append(
                    remote(
                        src.at[:, columns], dst.at[my_rows, pl.ds(h * HEAD, HEAD)],
                        qe_send.at[i, h, n], qe_recv.at[i, h, mine], device,
                    )
                )
                sends[-1].start()
        if h == 0:
            loads[3].wait()
            loads[4].wait()
            lane = lax.broadcasted_iota(jnp.int32, (TOK, HEAD), 1)
            delta = jnp.zeros((TOK, HEAD), F32)
            for head in range(PIECES * GROUP):
                part = pl.ds(head * HEAD, HEAD)
                product = e_src[:, part].astype(F32) * o_src[:, part].astype(F32)
                delta = jnp.where(lane == head, jnp.sum(product, axis=1, keepdims=True), delta)
            delta = delta.T
            lse = lse_ref[...] * LOG2E + SHIFT
            for g in range(PIECES):
                aux_src[g, 0:GROUP, :] = lse[g * GROUP : (g + 1) * GROUP, :]
                aux_src[g, GROUP : 2 * GROUP, :] = delta[g * GROUP : (g + 1) * GROUP, :]
            for n, device, g in peers:
                sends.append(remote(aux_src.at[g], aux.at[mine], aux_send.at[n], aux_recv.at[mine], device))
                sends[-1].start()
            aux[mine] = aux_src[group]

    def halo_copies(by, piece):
        rows = pl.ds(pl.multiple_of(HALO + piece * TOK, TOK), TOK)
        to = pl.ds(pl.multiple_of((HALF if by == 1 else -HALF) + piece * TOK, TOK), TOK)
        at = piece if by == 1 else piece + Y
        return [
            remote(ref.at[rows, :], ref.at[to, :], halo_send.at[i, at], halo_recv.at[i, at], span_device(by))
            for i, ref in enumerate((k_all, v_all))
        ]

    def start_all(copies):
        for copy in copies:
            copy.start()

    def here(ref, sem):
        return pltpu.make_async_copy(ref, ref, sem)

    for dy, dcore in ((0, 0), (0, 1), (1, 0), (3, 0), (1, 1), (3, 1), (2, 0), (2, 1)):
        piece = lax.rem(core + dcore, 2) * Y + lax.rem(y + dy, Y)
        rows = pl.ds(pl.multiple_of(HALO + piece * TOK, TOK), TOK)
        here(k_all.at[rows, :], kv_recv.at[0, piece]).wait()
        here(v_all.at[rows, :], kv_recv.at[1, piece]).wait()
        pl.when(has_next)(lambda: start_all(halo_copies(1, piece)))
    for piece in range(Y, PIECES):
        pl.when(has_next2)(lambda: start_all(halo_copies(2, piece)))

    loads[5].wait()
    first = span * PIECES - HALO // TOK
    for i in range((HALO + SPAN) // TOK):
        row = seg_ref[pl.ds(jnp.maximum(first + i, 0), 1), :]
        row = jnp.where(first + i < 0, -1, row)
        seg_k[pl.ds(i * TOK, TOK), :] = jnp.broadcast_to(row, (TOK, TOK)).T
        if i >= HALO // TOK:
            seg_q[:, pl.ds(i * TOK - HALO, TOK)] = row

    dk_acc[...] = jnp.zeros_like(dk_acc)
    dv_acc[...] = jnp.zeros_like(dv_acc)
    dq_t[...] = jnp.zeros_like(dq_t)

    for piece in range(PIECES):
        pl.when(mine != piece)(lambda: here(aux.at[piece], aux_recv.at[piece]).wait())

    def step(j, h, r0, r1):
        keys = pl.ds(j * BLOCK, BLOCK)
        width = (r1 - r0) * BLOCK
        rows = pl.ds(r0 * BLOCK, width)
        columns = pl.ds(pl.multiple_of(h * HEAD, HEAD), HEAD)
        q, e = q_all[rows, columns], e_all[rows, columns]
        k, v = k_all[keys, :], v_all[keys, :]
        scores = lax.dot_general(k, q, NT, preferred_element_type=F32)
        dprobs = lax.dot_general(v, e, NT, preferred_element_type=F32)
        pieces = range(r0 * BLOCK // TOK, r1 * BLOCK // TOK)
        lse = jnp.concatenate([aux[p, pl.ds(h, 1), :] for p in pieces], axis=1)
        delta = jnp.concatenate([aux[p, pl.ds(h + GROUP, 1), :] for p in pieces], axis=1)
        doc = jnp.concatenate([seg_k[keys, :]] * (width // TOK), axis=1)
        allowed = doc == seg_q[:, rows]
        if j >= HALO_BLOCKS:
            key_at = lax.broadcasted_iota(jnp.int32, (BLOCK, width), 0) + (j - HALO_BLOCKS) * BLOCK
            query_at = lax.broadcasted_iota(jnp.int32, (BLOCK, width), 1) + r0 * BLOCK
            allowed = allowed & (key_at <= query_at)
        probs = jnp.exp2(jnp.where(allowed, scores * (SCALE * LOG2E) - lse, -jnp.inf))
        dscores = (probs * (dprobs - delta)).astype(BF16)
        probs = probs.astype(BF16)
        dv_acc[keys, :] += jnp.dot(probs, e, preferred_element_type=F32)
        dk_acc[keys, :] += jnp.dot(dscores, q, preferred_element_type=F32)
        dq_t[h, :, rows] += lax.dot_general(k, dscores, TN, preferred_element_type=F32)

    def wait_head(h):
        columns = pl.ds(pl.multiple_of(h * HEAD, HEAD), HEAD)
        for piece in range(PIECES):
            rows = pl.ds(piece * TOK, TOK)
            here(q_all.at[rows, columns], qe_recv.at[0, h, piece]).wait()
            here(e_all.at[rows, columns], qe_recv.at[1, h, piece]).wait()

    def wait_halo(pieces, by):
        for piece in pieces:
            at = piece if by == 1 else piece + Y
            rows = pl.ds((HALF if by == 1 else -HALF) + piece * TOK, TOK)
            here(k_all.at[rows, :], halo_recv.at[0, at]).wait()
            here(v_all.at[rows, :], halo_recv.at[1, at]).wait()

    def own(h):
        for b in range(SPAN_BLOCKS):
            step(HALO_BLOCKS + b, h, b, SPAN_BLOCKS)

    def halo(h, blocks):
        for j in blocks:
            step(j, h, 0, min(SPAN_BLOCKS, j + 1))

    near_blocks = tuple(reversed(range(HALF // BLOCK, HALO_BLOCKS)))
    far_blocks = tuple(reversed(range(HALF // BLOCK)))

    def dq_copy(h, piece):
        columns = pl.ds(pl.multiple_of(h * HEAD, HEAD), HEAD)
        out_columns = pl.ds(pl.multiple_of(group * QCOLS + h * HEAD, HEAD), HEAD)
        return remote(
            dq_send.at[pl.ds(piece * TOK, TOK), columns], dq_out.at[:, out_columns],
            dq_send_sem.at[h, piece], dq_recv_sem.at[h, group], piece_device(piece),
        )

    def dq_local(h, piece):
        columns = pl.ds(pl.multiple_of(h * HEAD, HEAD), HEAD)
        out_columns = pl.ds(pl.multiple_of(group * QCOLS + h * HEAD, HEAD), HEAD)
        return pltpu.make_async_copy(
            dq_send.at[pl.ds(piece * TOK, TOK), columns], dq_out.at[:, out_columns], dq_recv_sem.at[h, group]
        )

    def finish_head(h):
        columns = pl.ds(pl.multiple_of(h * HEAD, HEAD), HEAD)
        dq_send[:, columns] = (dq_t[h].T * REST).astype(BF16)
        for piece in range(PIECES):
            pl.when(mine != piece)(lambda: dq_copy(h, piece).start())
            pl.when(mine == piece)(lambda: dq_local(h, piece).start())

    def far_and_finish(h, carry):
        pl.when(has_prev2)(lambda: halo(h, far_blocks))
        finish_head(h)
        return carry

    def early_head(h, carry):
        wait_head(h)
        own(h)
        pl.when(has_prev & (h == 0))(lambda: wait_halo(range(PIECES), 1))
        pl.when(has_prev)(lambda: halo(h, near_blocks))
        pl.when(has_prev2 & (h == 1))(lambda: wait_halo(range(Y, PIECES), 2))
        return lax.fori_loop(h // 2 * 2, h + (h + 1) // 2, far_and_finish, carry)

    lax.fori_loop(0, GROUP - 1, early_head, 0)

    def back_copies(j):
        rows = pl.ds(j * BLOCK, BLOCK)
        if j * BLOCK >= HALF:
            dsts, at, by = (dk_near, dv_near), pl.ds(j * BLOCK - HALF, BLOCK), -1
        else:
            dsts, at, by = (dk_far, dv_far), rows, -2
        return [
            remote(src.at[rows, :], dst.at[at, :], back_send.at[i, j], back_recv.at[i, j], span_device(by))
            for i, (src, dst) in enumerate(((dk_back, dsts[0]), (dv_back, dsts[1])))
        ]

    def last_halo(blocks):
        for j in blocks:
            rows = pl.ds(j * BLOCK, BLOCK)
            halo(GROUP - 1, (j,))
            dk_back[rows, :] = (dk_acc[rows, :] * REST).astype(BF16)
            dv_back[rows, :] = (dv_acc[rows, :] * 2.0**SHIFT).astype(BF16)
            start_all(back_copies(j))

    wait_head(GROUP - 1)
    pl.when(has_prev2)(lambda: last_halo(far_blocks))
    pl.when(has_prev)(lambda: last_halo(near_blocks))
    own(GROUP - 1)
    finish_head(GROUP - 1)

    def dkv_copies(piece):
        rows = pl.ds(piece * TOK, TOK)
        return [
            remote(
                src.at[rows, :], dst.at[:, cols(group, HEAD)],
                dkv_send_sem.at[i, piece], dkv_recv_sem.at[i, group], piece_device(piece),
            )
            for i, src, dst in ((0, dk_send, dk_out), (1, dv_send, dv_out))
        ]

    def dkv_local(piece):
        rows = pl.ds(piece * TOK, TOK)
        return [
            pltpu.make_async_copy(src.at[rows, :], dst.at[:, cols(group, HEAD)], dkv_recv_sem.at[i, group])
            for i, src, dst in ((0, dk_send, dk_out), (1, dv_send, dv_out))
        ]

    def finish_keys(b):
        rows = pl.ds(b * BLOCK, BLOCK)
        acc_rows = pl.ds(HALO + b * BLOCK, BLOCK)
        for i, acc, near, far, out, factor in (
            (0, dk_acc, dk_near, dk_far, dk_send, REST),
            (1, dv_acc, dv_near, dv_far, dv_send, 2.0**SHIFT),
        ):
            acc[acc_rows, :] *= factor

            def add_near():
                here(near.at[rows, :], back_recv.at[i, b + HALF // BLOCK]).wait()
                acc[acc_rows, :] += near[rows, :].astype(F32)

            def add_far():
                far_rows = pl.ds(b * BLOCK - HALF, BLOCK)
                here(far.at[far_rows, :], back_recv.at[i, b - HALF // BLOCK]).wait()
                acc[acc_rows, :] += far[far_rows, :].astype(F32)

            pl.when(has_next)(add_near)
            if b * BLOCK >= HALF:
                pl.when(has_next2)(add_far)
            out[rows, :] = acc[acc_rows, :].astype(BF16)
        for piece in (2 * b, 2 * b + 1):
            pl.when(mine != piece)(lambda: start_all(dkv_copies(piece)))
            pl.when(mine == piece)(lambda: start_all(dkv_local(piece)))

    for b in reversed(range(SPAN_BLOCKS)):
        finish_keys(b)

    for g in range(PIECES):
        for h in range(GROUP):
            here(dq_out.at[:, pl.ds(g * QCOLS + h * HEAD, HEAD)], dq_recv_sem.at[h, g]).wait()
        here(dk_out.at[:, pl.ds(g * HEAD, HEAD)], dkv_recv_sem.at[0, g]).wait()
        here(dv_out.at[:, pl.ds(g * HEAD, HEAD)], dkv_recv_sem.at[1, g]).wait()
    for copy in sends:
        copy.wait_send()

    def wait_sends(copies):
        for copy in copies:
            copy.wait_send()

    for piece in range(PIECES):
        pl.when(has_next)(lambda: wait_sends(halo_copies(1, piece)))
        if piece >= Y:
            pl.when(has_next2)(lambda: wait_sends(halo_copies(2, piece)))
        pl.when(mine != piece)(lambda: wait_sends([dq_copy(h, piece) for h in range(GROUP)] + dkv_copies(piece)))
    for j in range(HALO_BLOCKS):
        pl.when(has_prev if j * BLOCK >= HALF else has_prev2)(lambda: wait_sends(back_copies(j)))


def shards(n_span, query, key, value, out, output_gradient, log_sum_exp, segment_ids):
    hbm = pl.BlockSpec(memory_space=pltpu.HBM)
    dma = pltpu.SemaphoreType.DMA
    shape = jax.ShapeDtypeStruct
    window = HALO + SPAN
    return pl.pallas_call(
        functools.partial(kernel, n_span),
        out_shape=[
            shape(query.shape, BF16),
            shape(key.shape, BF16),
            shape(value.shape, BF16),
        ],
        in_specs=[hbm] * 7,
        out_specs=[hbm] * 3,
        scratch_shapes=[
            pltpu.VMEM((TOK, PIECES * HEAD), BF16),
            pltpu.VMEM((TOK, PIECES * HEAD), BF16),
            pltpu.VMEM((TOK, PIECES * QCOLS), BF16),
            pltpu.VMEM((TOK, PIECES * QCOLS), BF16),
            pltpu.VMEM((PIECES * GROUP, TOK), F32),
            pltpu.VMEM((segment_ids.shape[0] // TOK, TOK), jnp.int32),
            pltpu.VMEM((PIECES, 2 * GROUP, TOK), F32),
            pltpu.VMEM((window, HEAD), BF16),
            pltpu.VMEM((window, HEAD), BF16),
            pltpu.VMEM((SPAN, QCOLS), BF16),
            pltpu.VMEM((SPAN, QCOLS), BF16),
            pltpu.VMEM((PIECES, 2 * GROUP, TOK), F32),
            pltpu.VMEM((window, TOK), jnp.int32),
            pltpu.VMEM((1, SPAN), jnp.int32),
            pltpu.VMEM((GROUP, HEAD, SPAN), F32),
            pltpu.VMEM((window, HEAD), F32),
            pltpu.VMEM((window, HEAD), F32),
            pltpu.VMEM((SPAN, QCOLS), BF16),
            pltpu.VMEM((SPAN, HEAD), BF16),
            pltpu.VMEM((SPAN, HEAD), BF16),
            pltpu.VMEM((HALO, HEAD), BF16),
            pltpu.VMEM((HALO, HEAD), BF16),
            pltpu.VMEM((SPAN, HEAD), BF16),
            pltpu.VMEM((SPAN, HEAD), BF16),
            pltpu.VMEM((HALF, HEAD), BF16),
            pltpu.VMEM((HALF, HEAD), BF16),
            dma((6,)),
            dma((2, PIECES)),
            dma((2, PIECES)),
            dma((PIECES,)),
            dma((PIECES,)),
            dma((2, GROUP, PIECES)),
            dma((2, GROUP, PIECES)),
            dma((2, PIECES + Y)),
            dma((2, PIECES + Y)),
            dma((2, HALO_BLOCKS)),
            dma((2, HALO_BLOCKS)),
            dma((GROUP, PIECES)),
            dma((GROUP, PIECES)),
            dma((2, PIECES)),
            dma((2, PIECES)),
        ],
        name="attention_backward",
        compiler_params=pltpu.CompilerParams(
            collective_id=0, has_side_effects=True, vmem_limit_bytes=67_043_328
        ),
    )(query, key, value, out, output_gradient, log_sum_exp.T, segment_ids.reshape(-1, TOK))


def solution(mesh):
    rows = P(("seq", "head"), None)
    return jax.shard_map(
        functools.partial(shards, mesh.shape["seq"] // 2),
        mesh=mesh,
        in_specs=(rows,) * 6 + (P(),),
        out_specs=(rows,) * 3,
        check_vma=False,
    )
```

```python
import functools
import math

import jax
import jax.numpy as jnp
from jax import lax
from jax.experimental import pallas as pl
from jax.experimental.pallas import tpu as pltpu
from jax.sharding import PartitionSpec as P

MESH = pl.DeviceIdType.MESH
BF16 = jnp.bfloat16
F32 = jnp.float32

HEAD = 128
TOK = 128
GROUP = 4
Y = 4
PIECES = 8
SPAN = PIECES * TOK
HALF = SPAN // 2
HALO = SPAN + HALF
BLOCK = 256
HALO_BLOCKS = HALO // BLOCK
SPAN_BLOCKS = SPAN // BLOCK
QCOLS = GROUP * HEAD

LOG2E = math.log2(math.e)
SCALE = 1.0 / math.sqrt(HEAD)
SHIFT = 4.0
REST = SCALE * 2.0**SHIFT
NT = (((1,), (1,)), ((), ()))
TN = (((0,), (0,)), ((), ()))


def kernel(
    n_span,
    q_hbm, k_hbm, v_hbm, o_hbm, e_hbm, lse_hbm, seg_hbm,
    dq_out, dk_out, dv_out,
    k_src, v_src, o_src, e_src, lse_ref, seg_ref, aux_src,
    k_all, v_all, q_all, e_all, aux, seg_k, seg_q,
    dq_t, dk_acc, dv_acc,
    dq_send, dk_send, dv_send, dk_back, dv_back, dk_near, dv_near, dk_far, dv_far,
    load_sem, kv_send, kv_recv, aux_send, aux_recv, qe_send, qe_recv,
    halo_send, halo_recv, back_send, back_recv,
    dq_send_sem, dq_recv_sem, dkv_send_sem, dkv_recv_sem,
):
    seq = lax.axis_index("seq")
    y = lax.axis_index("head")
    span = lax.div(seq, 2)
    core = lax.rem(seq, 2)
    mine = core * Y + y
    group = y * 2 + core

    def piece_device(piece):
        return (span * 2 + piece // Y, piece % Y)

    def span_device(by):
        return (seq + 2 * by, y)

    peers = []
    for dy in (1, 3, 2, 0):
        for dcore in (0, 1):
            if dy or dcore:
                py = lax.rem(y + dy, Y)
                pcore = lax.rem(core + dcore, 2)
                peers.append((dy * 2 + dcore, (span * 2 + pcore, py), py * 2 + pcore))

    has_prev, has_prev2 = span >= 1, span >= 2
    has_next, has_next2 = span < n_span - 1, span < n_span - 2

    def cols(g, width):
        return pl.ds(pl.multiple_of(g * width, width), width)

    my_rows = pl.ds(pl.multiple_of(mine * TOK, TOK), TOK)
    my_key_rows = pl.ds(pl.multiple_of(HALO + mine * TOK, TOK), TOK)
    loads = [
        pltpu.make_async_copy(src, dst, load_sem.at[i])
        for i, (src, dst) in enumerate(
            (
                (k_hbm, k_src), (v_hbm, v_src), (e_hbm, e_src), (o_hbm, o_src),
                (lse_hbm, lse_ref), (seg_hbm, seg_ref),
            )
        )
    ]
    own = [
        pltpu.make_async_copy(k_hbm.at[:, cols(group, HEAD)], k_all.at[my_key_rows, :], kv_recv.at[0, mine]),
        pltpu.make_async_copy(v_hbm.at[:, cols(group, HEAD)], v_all.at[my_key_rows, :], kv_recv.at[1, mine]),
    ]
    for h in range(GROUP):
        columns = pl.ds(pl.multiple_of(group * QCOLS + h * HEAD, HEAD), HEAD)
        for i, (src, dst) in enumerate(((q_hbm, q_all), (e_hbm, e_all))):
            own.append(
                pltpu.make_async_copy(
                    src.at[:, columns], dst.at[my_rows, pl.ds(h * HEAD, HEAD)], qe_recv.at[i, h, mine]
                )
            )
    for copy in loads + own:
        copy.start()

    barrier = pltpu.get_barrier_semaphore()

    def greet(device):
        pl.semaphore_signal(barrier, inc=1, device_id=device, device_id_type=MESH)

    for _, device, _ in peers:
        greet(device)
    pl.when(has_prev)(lambda: greet(span_device(-1)))
    pl.when(has_prev2)(lambda: greet(span_device(-2)))
    pl.when(has_next)(lambda: greet(span_device(1)))
    pl.when(has_next2)(lambda: greet(span_device(2)))
    neighbours = jnp.minimum(span, 2) + jnp.minimum(n_span - 1 - span, 2)
    pl.semaphore_wait(barrier, len(peers) + neighbours)

    def remote(src, dst, send, recv, device):
        return pltpu.make_async_remote_copy(
            src_ref=src, dst_ref=dst, send_sem=send, recv_sem=recv, device_id=device, device_id_type=MESH
        )

    sends = []
    loads[0].wait()
    loads[1].wait()
    for n, device, g in peers:
        for i, (src, dst) in enumerate(((k_src, k_all), (v_src, v_all))):
            sends.append(
                remote(src.at[:, cols(g, HEAD)], dst.at[my_key_rows, :], kv_send.at[i, n], kv_recv.at[i, mine], device)
            )
            sends[-1].start()

    def qe_copies(h):
        copies = []
        for n, device, g in peers:
            columns = pl.ds(pl.multiple_of(g * QCOLS + h * HEAD, HEAD), HEAD)
            at_columns = pl.ds(pl.multiple_of(h * HEAD, HEAD), HEAD)
            for i, (src, dst) in enumerate(((q_hbm, q_all), (e_src, e_all))):
                copies.append(
                    remote(
                        src.at[:, columns], dst.at[my_rows, at_columns],
                        qe_send.at[i, h, n], qe_recv.at[i, h, mine], device,
                    )
                )
        return copies

    def start_all(copies):
        for copy in copies:
            copy.start()

    loads[2].wait()
    pl.when(core == 0)(lambda: start_all(qe_copies(0)))

    loads[3].wait()
    loads[4].wait()
    lane = lax.broadcasted_iota(jnp.int32, (TOK, HEAD), 1)
    delta = jnp.zeros((TOK, HEAD), F32)
    for head in range(PIECES * GROUP):
        part = pl.ds(head * HEAD, HEAD)
        product = e_src[:, part].astype(F32) * o_src[:, part].astype(F32)
        delta = jnp.where(lane == head, jnp.sum(product, axis=1, keepdims=True), delta)
    delta = delta.T
    lse = lse_ref[...] * LOG2E + SHIFT
    for g in range(PIECES):
        aux_src[g, 0:GROUP, :] = lse[g * GROUP : (g + 1) * GROUP, :]
        aux_src[g, GROUP : 2 * GROUP, :] = delta[g * GROUP : (g + 1) * GROUP, :]
    for n, device, g in peers:
        sends.append(remote(aux_src.at[g], aux.at[mine], aux_send.at[n], aux_recv.at[mine], device))
        sends[-1].start()
    aux[mine] = aux_src[group]
    pl.when(core == 0)(lambda: [start_all(qe_copies(h)) for h in range(1, GROUP)] and None)

    def halo_copies(by, piece):
        rows = pl.ds(pl.multiple_of(HALO + piece * TOK, TOK), TOK)
        to = pl.ds(pl.multiple_of((HALF if by == 1 else -HALF) + piece * TOK, TOK), TOK)
        at = piece if by == 1 else piece + Y
        return [
            remote(ref.at[rows, :], ref.at[to, :], halo_send.at[i, at], halo_recv.at[i, at], span_device(by))
            for i, ref in enumerate((k_all, v_all))
        ]

    def here(ref, sem):
        return pltpu.make_async_copy(ref, ref, sem)

    for dy, dcore in ((0, 0), (0, 1), (1, 0), (3, 0), (1, 1), (3, 1), (2, 0), (2, 1)):
        piece = lax.rem(core + dcore, 2) * Y + lax.rem(y + dy, Y)
        rows = pl.ds(pl.multiple_of(HALO + piece * TOK, TOK), TOK)
        here(k_all.at[rows, :], kv_recv.at[0, piece]).wait()
        here(v_all.at[rows, :], kv_recv.at[1, piece]).wait()
        pl.when(has_next)(lambda: start_all(halo_copies(1, piece)))
    for piece in range(Y, PIECES):
        pl.when(has_next2)(lambda: start_all(halo_copies(2, piece)))

    loads[5].wait()
    first = span * PIECES - HALO // TOK
    for i in range((HALO + SPAN) // TOK):
        row = seg_ref[pl.ds(jnp.maximum(first + i, 0), 1), :]
        row = jnp.where(first + i < 0, -1, row)
        seg_k[pl.ds(i * TOK, TOK), :] = jnp.broadcast_to(row, (TOK, TOK)).T
        if i >= HALO // TOK:
            seg_q[:, pl.ds(i * TOK - HALO, TOK)] = row

    dk_acc[...] = jnp.zeros_like(dk_acc)
    dv_acc[...] = jnp.zeros_like(dv_acc)
    dq_t[...] = jnp.zeros_like(dq_t)

    for piece in range(Y):
        pl.when(mine != piece)(lambda: here(aux.at[piece], aux_recv.at[piece]).wait())

    def step(j, blocks, h, r0, r1):
        keys = pl.ds(j * BLOCK, blocks * BLOCK)
        height, width = blocks * BLOCK, (r1 - r0) * BLOCK
        rows = pl.ds(r0 * BLOCK, width)
        columns = pl.ds(pl.multiple_of(h * HEAD, HEAD), HEAD)
        q, e = q_all[rows, columns], e_all[rows, columns]
        k, v = k_all[keys, :], v_all[keys, :]
        scores = lax.dot_general(k, q, NT, preferred_element_type=F32)
        dprobs = lax.dot_general(v, e, NT, preferred_element_type=F32)
        pieces = range(r0 * BLOCK // TOK, r1 * BLOCK // TOK)
        lse = jnp.concatenate([aux[p, pl.ds(h, 1), :] for p in pieces], axis=1)
        delta = jnp.concatenate([aux[p, pl.ds(h + GROUP, 1), :] for p in pieces], axis=1)
        doc = jnp.concatenate([seg_k[keys, :]] * (width // TOK), axis=1)
        allowed = doc == seg_q[:, rows]
        if j + blocks - 1 - HALO_BLOCKS >= r0:
            key_at = lax.broadcasted_iota(jnp.int32, (height, width), 0) + (j - HALO_BLOCKS) * BLOCK
            query_at = lax.broadcasted_iota(jnp.int32, (height, width), 1) + r0 * BLOCK
            allowed = allowed & (key_at <= query_at)
        probs = jnp.exp2(jnp.where(allowed, scores * (SCALE * LOG2E) - lse, -jnp.inf))
        dscores = (probs * (dprobs - delta)).astype(BF16)
        probs = probs.astype(BF16)
        dv_acc[keys, :] += jnp.dot(probs, e, preferred_element_type=F32)
        dk_acc[keys, :] += jnp.dot(dscores, q, preferred_element_type=F32)
        dq_t[h, :, rows] += lax.dot_general(k, dscores, TN, preferred_element_type=F32)

    def wait_head(h, pieces):
        columns = pl.ds(pl.multiple_of(h * HEAD, HEAD), HEAD)
        for piece in pieces:
            rows = pl.ds(piece * TOK, TOK)
            here(q_all.at[rows, columns], qe_recv.at[0, h, piece]).wait()
            here(e_all.at[rows, columns], qe_recv.at[1, h, piece]).wait()

    def wait_halo(pieces, by):
        for piece in pieces:
            at = piece if by == 1 else piece + Y
            rows = pl.ds((HALF if by == 1 else -HALF) + piece * TOK, TOK)
            here(k_all.at[rows, :], halo_recv.at[0, at]).wait()
            here(v_all.at[rows, :], halo_recv.at[1, at]).wait()

    low, high = range(Y), range(Y, PIECES)

    def run(h, steps):
        for j, blocks, r0, r1 in steps:
            step(j, blocks, h, r0, r1)

    own_low = ((6, 1, 0, 2), (7, 1, 1, 2))
    near_low = ((4, 2, 0, 2), (2, 2, 0, 2))
    far_low = ((1, 1, 0, 2), (0, 1, 0, 1))
    near_high = ((2, 1, 2, 3), (3, 1, 2, 4), (4, 2, 2, 4))
    own_high = ((6, 2, 2, 4), (8, 1, 2, 4), (9, 1, 3, 4))

    def dq_copy(h, piece):
        columns = pl.ds(pl.multiple_of(h * HEAD, HEAD), HEAD)
        out_columns = pl.ds(pl.multiple_of(group * QCOLS + h * HEAD, HEAD), HEAD)
        return remote(
            dq_send.at[pl.ds(piece * TOK, TOK), columns], dq_out.at[:, out_columns],
            dq_send_sem.at[h, piece], dq_recv_sem.at[h, group], piece_device(piece),
        )

    def dq_local(h, piece):
        columns = pl.ds(pl.multiple_of(h * HEAD, HEAD), HEAD)
        out_columns = pl.ds(pl.multiple_of(group * QCOLS + h * HEAD, HEAD), HEAD)
        return pltpu.make_async_copy(
            dq_send.at[pl.ds(piece * TOK, TOK), columns], dq_out.at[:, out_columns], dq_recv_sem.at[h, group]
        )

    def finish_head(h, pieces):
        columns = pl.ds(pl.multiple_of(h * HEAD, HEAD), HEAD)
        rows = pl.ds(pieces[0] * TOK, HALF)
        dq_send[rows, columns] = (dq_t[h, :, rows].T * REST).astype(BF16)
        for piece in pieces:
            pl.when(mine != piece)(lambda: dq_copy(h, piece).start())
            pl.when(mine == piece)(lambda: dq_local(h, piece).start())

    def back_copies(j):
        rows = pl.ds(j * BLOCK, BLOCK)
        if j * BLOCK >= HALF:
            dsts, at, by = (dk_near, dv_near), pl.ds(j * BLOCK - HALF, BLOCK), -1
        else:
            dsts, at, by = (dk_far, dv_far), rows, -2
        return [
            remote(src.at[rows, :], dst.at[at, :], back_send.at[i, j], back_recv.at[i, j], span_device(by))
            for i, (src, dst) in enumerate(((dk_back, dsts[0]), (dv_back, dsts[1])))
        ]

    def send_back(j, blocks):
        rows = pl.ds(j * BLOCK, blocks * BLOCK)
        dk_back[rows, :] = (dk_acc[rows, :] * REST).astype(BF16)
        dv_back[rows, :] = (dv_acc[rows, :] * 2.0**SHIFT).astype(BF16)
        for at in range(j, j + blocks):
            start_all(back_copies(at))

    def low_head(h, carry):
        wait_head(h, low)
        pl.when((core == 1) & (h >= 1))(lambda: start_all(qe_copies(h - 1)))
        run(h, own_low)
        pl.when(has_prev & (h == 1))(lambda: wait_halo(range(PIECES), 1))
        pl.when(has_prev & (h >= 1))(lambda: run(h - 1, near_low))
        return carry

    lax.fori_loop(0, GROUP, low_head, 0)
    pl.when(core == 1)(lambda: start_all(qe_copies(GROUP - 1)))
    pl.when(has_prev)(lambda: run(GROUP - 1, near_low))
    pl.when(has_prev2)(lambda: wait_halo(high, 2))

    def far_head(h, carry):
        pl.when(has_prev2)(lambda: run(h, far_low))
        finish_head(h, low)
        return carry

    lax.fori_loop(0, GROUP, far_head, 0)
    pl.when(has_prev2)(lambda: send_back(0, 2))

    for piece in high:
        pl.when(mine != piece)(lambda: here(aux.at[piece], aux_recv.at[piece]).wait())

    def near_head(h, carry):
        wait_head(h, high)
        pl.when(has_prev)(lambda: run(h, near_high))
        return carry

    lax.fori_loop(0, GROUP - 1, near_head, 0)
    wait_head(GROUP - 1, high)

    def last_near():
        for j, blocks, r0, r1 in near_high:
            step(j, blocks, GROUP - 1, r0, r1)
            send_back(j, blocks)

    pl.when(has_prev)(last_near)

    def high_head(h, carry):
        run(h, own_high)
        finish_head(h, high)
        return carry

    lax.fori_loop(0, GROUP, high_head, 0)

    def dkv_copies(piece):
        rows = pl.ds(piece * TOK, TOK)
        return [
            remote(
                src.at[rows, :], dst.at[:, cols(group, HEAD)],
                dkv_send_sem.at[i, piece], dkv_recv_sem.at[i, group], piece_device(piece),
            )
            for i, src, dst in ((0, dk_send, dk_out), (1, dv_send, dv_out))
        ]

    def dkv_local(piece):
        rows = pl.ds(piece * TOK, TOK)
        return [
            pltpu.make_async_copy(src.at[rows, :], dst.at[:, cols(group, HEAD)], dkv_recv_sem.at[i, group])
            for i, src, dst in ((0, dk_send, dk_out), (1, dv_send, dv_out))
        ]

    def finish_keys(b):
        rows = pl.ds(b * BLOCK, BLOCK)
        acc_rows = pl.ds(HALO + b * BLOCK, BLOCK)
        for i, acc, near, far, out, factor in (
            (0, dk_acc, dk_near, dk_far, dk_send, REST),
            (1, dv_acc, dv_near, dv_far, dv_send, 2.0**SHIFT),
        ):
            acc[acc_rows, :] *= factor

            def add_near():
                here(near.at[rows, :], back_recv.at[i, b + HALF // BLOCK]).wait()
                acc[acc_rows, :] += near[rows, :].astype(F32)

            def add_far():
                far_rows = pl.ds(b * BLOCK - HALF, BLOCK)
                here(far.at[far_rows, :], back_recv.at[i, b - HALF // BLOCK]).wait()
                acc[acc_rows, :] += far[far_rows, :].astype(F32)

            pl.when(has_next)(add_near)
            if b * BLOCK >= HALF:
                pl.when(has_next2)(add_far)
            out[rows, :] = acc[acc_rows, :].astype(BF16)
        for piece in (2 * b, 2 * b + 1):
            pl.when(mine != piece)(lambda: start_all(dkv_copies(piece)))
            pl.when(mine == piece)(lambda: start_all(dkv_local(piece)))

    for b in range(SPAN_BLOCKS):
        finish_keys(b)

    for g in range(PIECES):
        for h in range(GROUP):
            here(dq_out.at[:, pl.ds(g * QCOLS + h * HEAD, HEAD)], dq_recv_sem.at[h, g]).wait()
        here(dk_out.at[:, pl.ds(g * HEAD, HEAD)], dkv_recv_sem.at[0, g]).wait()
        here(dv_out.at[:, pl.ds(g * HEAD, HEAD)], dkv_recv_sem.at[1, g]).wait()
    def wait_sends(copies):
        for copy in copies:
            copy.wait_send()

    wait_sends(sends)
    for h in range(GROUP):
        wait_sends(qe_copies(h))

    for piece in range(PIECES):
        pl.when(has_next)(lambda: wait_sends(halo_copies(1, piece)))
        if piece >= Y:
            pl.when(has_next2)(lambda: wait_sends(halo_copies(2, piece)))
        pl.when(mine != piece)(lambda: wait_sends([dq_copy(h, piece) for h in range(GROUP)] + dkv_copies(piece)))
    for j in range(HALO_BLOCKS):
        pl.when(has_prev if j * BLOCK >= HALF else has_prev2)(lambda: wait_sends(back_copies(j)))


def shards(n_span, query, key, value, out, output_gradient, log_sum_exp, segment_ids):
    hbm = pl.BlockSpec(memory_space=pltpu.HBM)
    dma = pltpu.SemaphoreType.DMA
    shape = jax.ShapeDtypeStruct
    window = HALO + SPAN
    return pl.pallas_call(
        functools.partial(kernel, n_span),
        out_shape=[
            shape(query.shape, BF16),
            shape(key.shape, BF16),
            shape(value.shape, BF16),
        ],
        in_specs=[hbm] * 7,
        out_specs=[hbm] * 3,
        scratch_shapes=[
            pltpu.VMEM((TOK, PIECES * HEAD), BF16),
            pltpu.VMEM((TOK, PIECES * HEAD), BF16),
            pltpu.VMEM((TOK, PIECES * QCOLS), BF16),
            pltpu.VMEM((TOK, PIECES * QCOLS), BF16),
            pltpu.VMEM((PIECES * GROUP, TOK), F32),
            pltpu.VMEM((segment_ids.shape[0] // TOK, TOK), jnp.int32),
            pltpu.VMEM((PIECES, 2 * GROUP, TOK), F32),
            pltpu.VMEM((window, HEAD), BF16),
            pltpu.VMEM((window, HEAD), BF16),
            pltpu.VMEM((SPAN, QCOLS), BF16),
            pltpu.VMEM((SPAN, QCOLS), BF16),
            pltpu.VMEM((PIECES, 2 * GROUP, TOK), F32),
            pltpu.VMEM((window, TOK), jnp.int32),
            pltpu.VMEM((1, SPAN), jnp.int32),
            pltpu.VMEM((GROUP, HEAD, SPAN), F32),
            pltpu.VMEM((window, HEAD), F32),
            pltpu.VMEM((window, HEAD), F32),
            pltpu.VMEM((SPAN, QCOLS), BF16),
            pltpu.VMEM((SPAN, HEAD), BF16),
            pltpu.VMEM((SPAN, HEAD), BF16),
            pltpu.VMEM((HALO, HEAD), BF16),
            pltpu.VMEM((HALO, HEAD), BF16),
            pltpu.VMEM((SPAN, HEAD), BF16),
            pltpu.VMEM((SPAN, HEAD), BF16),
            pltpu.VMEM((HALF, HEAD), BF16),
            pltpu.VMEM((HALF, HEAD), BF16),
            dma((6,)),
            dma((2, PIECES)),
            dma((2, PIECES)),
            dma((PIECES,)),
            dma((PIECES,)),
            dma((2, GROUP, PIECES)),
            dma((2, GROUP, PIECES)),
            dma((2, PIECES + Y)),
            dma((2, PIECES + Y)),
            dma((2, HALO_BLOCKS)),
            dma((2, HALO_BLOCKS)),
            dma((GROUP, PIECES)),
            dma((GROUP, PIECES)),
            dma((2, PIECES)),
            dma((2, PIECES)),
        ],
        name="attention_backward",
        compiler_params=pltpu.CompilerParams(
            collective_id=0, has_side_effects=True, vmem_limit_bytes=67_043_328
        ),
    )(query, key, value, out, output_gradient, log_sum_exp.T, segment_ids.reshape(-1, TOK))


def solution(mesh):
    rows = P(("seq", "head"), None)
    return jax.shard_map(
        functools.partial(shards, mesh.shape["seq"] // 2),
        mesh=mesh,
        in_specs=(rows,) * 6 + (P(),),
        out_specs=(rows,) * 3,
        check_vma=False,
    )
```

```python
import functools
import math

import jax
import jax.numpy as jnp
from jax import lax
from jax.experimental import pallas as pl
from jax.experimental.pallas import tpu as pltpu
from jax.sharding import PartitionSpec as P

MESH = pl.DeviceIdType.MESH
BF16 = jnp.bfloat16
F32 = jnp.float32

HEAD = 128
TOK = 128
GROUP = 4
Y = 4
PIECES = 8
SPAN = PIECES * TOK
HALF = SPAN // 2
HALO = SPAN + HALF
BLOCK = 256
HALO_BLOCKS = HALO // BLOCK
SPAN_BLOCKS = SPAN // BLOCK
QCOLS = GROUP * HEAD

LOG2E = math.log2(math.e)
SCALE = 1.0 / math.sqrt(HEAD)
SHIFT = 4.0
REST = SCALE * 2.0**SHIFT
NT = (((1,), (1,)), ((), ()))
TN = (((0,), (0,)), ((), ()))


def kernel(
    n_span,
    q_hbm, k_hbm, v_hbm, o_hbm, e_hbm, lse_hbm, seg_hbm,
    dq_out, dk_out, dv_out,
    k_src, v_src, o_src, e_src, lse_ref, seg_ref, aux_src,
    k_all, v_all, q_all, e_all, aux, seg_k, seg_q,
    dq_t, dk_acc, dv_acc,
    dq_send, dk_send, dv_send, dk_back, dv_back, dk_near, dv_near, dk_far, dv_far,
    load_sem, kv_send, kv_recv, aux_send, aux_recv, qe_send, qe_recv,
    halo_send, halo_recv, back_send, back_recv,
    dq_send_sem, dq_recv_sem, dkv_send_sem, dkv_recv_sem,
):
    seq = lax.axis_index("seq")
    y = lax.axis_index("head")
    span = lax.div(seq, 2)
    core = lax.rem(seq, 2)
    mine = core * Y + y
    group = y * 2 + core

    def piece_device(piece):
        return (span * 2 + piece // Y, piece % Y)

    def span_device(by):
        return (seq + 2 * by, y)

    peers = []
    for dy in (1, 3, 2, 0):
        for dcore in (0, 1):
            if dy or dcore:
                py = lax.rem(y + dy, Y)
                pcore = lax.rem(core + dcore, 2)
                peers.append((dy * 2 + dcore, (span * 2 + pcore, py), py * 2 + pcore))

    has_prev, has_prev2 = span >= 1, span >= 2
    has_next, has_next2 = span < n_span - 1, span < n_span - 2

    def cols(g, width):
        return pl.ds(pl.multiple_of(g * width, width), width)

    my_rows = pl.ds(pl.multiple_of(mine * TOK, TOK), TOK)
    my_key_rows = pl.ds(pl.multiple_of(HALO + mine * TOK, TOK), TOK)
    loads = [
        pltpu.make_async_copy(src, dst, load_sem.at[i])
        for i, (src, dst) in enumerate(
            (
                (k_hbm, k_src), (v_hbm, v_src), (e_hbm, e_src), (o_hbm, o_src),
                (lse_hbm, lse_ref), (seg_hbm, seg_ref),
            )
        )
    ]
    own = [
        pltpu.make_async_copy(k_hbm.at[:, cols(group, HEAD)], k_all.at[my_key_rows, :], kv_recv.at[0, mine]),
        pltpu.make_async_copy(v_hbm.at[:, cols(group, HEAD)], v_all.at[my_key_rows, :], kv_recv.at[1, mine]),
    ]
    for h in range(GROUP):
        columns = pl.ds(pl.multiple_of(group * QCOLS + h * HEAD, HEAD), HEAD)
        for i, (src, dst) in enumerate(((q_hbm, q_all), (e_hbm, e_all))):
            own.append(
                pltpu.make_async_copy(
                    src.at[:, columns], dst.at[my_rows, pl.ds(h * HEAD, HEAD)], qe_recv.at[i, h, mine]
                )
            )
    for copy in loads + own:
        copy.start()

    barrier = pltpu.get_barrier_semaphore()

    def greet(device):
        pl.semaphore_signal(barrier, inc=1, device_id=device, device_id_type=MESH)

    for _, device, _ in peers:
        greet(device)
    pl.when(has_prev)(lambda: greet(span_device(-1)))
    pl.when(has_prev2)(lambda: greet(span_device(-2)))
    pl.when(has_next)(lambda: greet(span_device(1)))
    pl.when(has_next2)(lambda: greet(span_device(2)))
    neighbours = jnp.minimum(span, 2) + jnp.minimum(n_span - 1 - span, 2)
    pl.semaphore_wait(barrier, len(peers) + neighbours)

    def remote(src, dst, send, recv, device):
        return pltpu.make_async_remote_copy(
            src_ref=src, dst_ref=dst, send_sem=send, recv_sem=recv, device_id=device, device_id_type=MESH
        )

    sends = []
    loads[0].wait()
    loads[1].wait()
    for n, device, g in peers:
        for i, (src, dst) in enumerate(((k_src, k_all), (v_src, v_all))):
            sends.append(
                remote(src.at[:, cols(g, HEAD)], dst.at[my_key_rows, :], kv_send.at[i, n], kv_recv.at[i, mine], device)
            )
            sends[-1].start()

    def qe_copies(h):
        copies = []
        for n, device, g in peers:
            columns = pl.ds(pl.multiple_of(g * QCOLS + h * HEAD, HEAD), HEAD)
            at_columns = pl.ds(pl.multiple_of(h * HEAD, HEAD), HEAD)
            for i, (src, dst) in enumerate(((q_hbm, q_all), (e_src, e_all))):
                copies.append(
                    remote(
                        src.at[:, columns], dst.at[my_rows, at_columns],
                        qe_send.at[i, h, n], qe_recv.at[i, h, mine], device,
                    )
                )
        return copies

    def start_all(copies):
        for copy in copies:
            copy.start()

    loads[2].wait()
    pl.when(core == 0)(lambda: start_all(qe_copies(0)))

    loads[3].wait()
    loads[4].wait()
    lane = lax.broadcasted_iota(jnp.int32, (TOK, HEAD), 1)
    delta = jnp.zeros((TOK, HEAD), F32)
    for head in range(PIECES * GROUP):
        part = pl.ds(head * HEAD, HEAD)
        product = e_src[:, part].astype(F32) * o_src[:, part].astype(F32)
        delta = jnp.where(lane == head, jnp.sum(product, axis=1, keepdims=True), delta)
    delta = delta.T
    lse = lse_ref[...] * LOG2E + SHIFT
    for g in range(PIECES):
        aux_src[g, 0:GROUP, :] = lse[g * GROUP : (g + 1) * GROUP, :]
        aux_src[g, GROUP : 2 * GROUP, :] = delta[g * GROUP : (g + 1) * GROUP, :]
    for n, device, g in peers:
        sends.append(remote(aux_src.at[g], aux.at[mine], aux_send.at[n], aux_recv.at[mine], device))
        sends[-1].start()
    aux[mine] = aux_src[group]
    pl.when(core == 0)(lambda: [start_all(qe_copies(h)) for h in range(1, GROUP)] and None)

    def halo_copies(by, piece):
        rows = pl.ds(pl.multiple_of(HALO + piece * TOK, TOK), TOK)
        to = pl.ds(pl.multiple_of((HALF if by == 1 else -HALF) + piece * TOK, TOK), TOK)
        at = piece if by == 1 else piece + Y
        return [
            remote(ref.at[rows, :], ref.at[to, :], halo_send.at[i, at], halo_recv.at[i, at], span_device(by))
            for i, ref in enumerate((k_all, v_all))
        ]

    def here(ref, sem):
        return pltpu.make_async_copy(ref, ref, sem)

    for dy, dcore in ((0, 0), (0, 1), (1, 0), (3, 0), (1, 1), (3, 1), (2, 0), (2, 1)):
        piece = lax.rem(core + dcore, 2) * Y + lax.rem(y + dy, Y)
        rows = pl.ds(pl.multiple_of(HALO + piece * TOK, TOK), TOK)
        here(k_all.at[rows, :], kv_recv.at[0, piece]).wait()
        here(v_all.at[rows, :], kv_recv.at[1, piece]).wait()
        pl.when(has_next)(lambda: start_all(halo_copies(1, piece)))
    for piece in range(Y, PIECES):
        pl.when(has_next2)(lambda: start_all(halo_copies(2, piece)))

    loads[5].wait()
    first = span * PIECES - HALO // TOK
    for i in range((HALO + SPAN) // TOK):
        row = seg_ref[pl.ds(jnp.maximum(first + i, 0), 1), :]
        row = jnp.where(first + i < 0, -1, row)
        seg_k[pl.ds(i * TOK, TOK), :] = jnp.broadcast_to(row, (TOK, TOK)).T
        if i >= HALO // TOK:
            seg_q[:, pl.ds(i * TOK - HALO, TOK)] = row

    dk_acc[...] = jnp.zeros_like(dk_acc)
    dv_acc[...] = jnp.zeros_like(dv_acc)
    dq_t[...] = jnp.zeros_like(dq_t)

    for piece in range(Y):
        pl.when(mine != piece)(lambda: here(aux.at[piece], aux_recv.at[piece]).wait())

    def where(j, blocks, h, r0, r1):
        keys = pl.ds(j * BLOCK, blocks * BLOCK)
        rows = pl.ds(r0 * BLOCK, (r1 - r0) * BLOCK)
        return keys, rows, pl.ds(pl.multiple_of(h * HEAD, HEAD), HEAD)

    def products(j, blocks, h, r0, r1):
        keys, rows, columns = where(j, blocks, h, r0, r1)
        scores = lax.dot_general(k_all[keys, :], q_all[rows, columns], NT, preferred_element_type=F32)
        dprobs = lax.dot_general(v_all[keys, :], e_all[rows, columns], NT, preferred_element_type=F32)
        return scores, dprobs

    def softmax_grad(j, blocks, h, r0, r1, scores, dprobs):
        keys, rows, _ = where(j, blocks, h, r0, r1)
        height, width = blocks * BLOCK, (r1 - r0) * BLOCK
        pieces = range(r0 * BLOCK // TOK, r1 * BLOCK // TOK)
        lse = jnp.concatenate([aux[p, pl.ds(h, 1), :] for p in pieces], axis=1)
        delta = jnp.concatenate([aux[p, pl.ds(h + GROUP, 1), :] for p in pieces], axis=1)
        doc = jnp.concatenate([seg_k[keys, :]] * (width // TOK), axis=1)
        allowed = doc == seg_q[:, rows]
        if j + blocks - 1 - HALO_BLOCKS >= r0:
            key_at = lax.broadcasted_iota(jnp.int32, (height, width), 0) + (j - HALO_BLOCKS) * BLOCK
            query_at = lax.broadcasted_iota(jnp.int32, (height, width), 1) + r0 * BLOCK
            allowed = allowed & (key_at <= query_at)
        probs = jnp.exp2(jnp.where(allowed, scores * (SCALE * LOG2E) - lse, -jnp.inf))
        return probs.astype(BF16), (probs * (dprobs - delta)).astype(BF16)

    def gradients(j, blocks, h, r0, r1, probs, dscores):
        keys, rows, columns = where(j, blocks, h, r0, r1)
        dv_acc[keys, :] += jnp.dot(probs, e_all[rows, columns], preferred_element_type=F32)
        dk_acc[keys, :] += jnp.dot(dscores, q_all[rows, columns], preferred_element_type=F32)
        dq_t[h, :, rows] += lax.dot_general(k_all[keys, :], dscores, TN, preferred_element_type=F32)

    def wait_head(h, pieces):
        columns = pl.ds(pl.multiple_of(h * HEAD, HEAD), HEAD)
        for piece in pieces:
            rows = pl.ds(piece * TOK, TOK)
            here(q_all.at[rows, columns], qe_recv.at[0, h, piece]).wait()
            here(e_all.at[rows, columns], qe_recv.at[1, h, piece]).wait()

    def wait_halo(pieces, by):
        for piece in pieces:
            at = piece if by == 1 else piece + Y
            rows = pl.ds((HALF if by == 1 else -HALF) + piece * TOK, TOK)
            here(k_all.at[rows, :], halo_recv.at[0, at]).wait()
            here(v_all.at[rows, :], halo_recv.at[1, at]).wait()

    low, high = range(Y), range(Y, PIECES)

    def run(h, steps, after=None):
        steps = [(j, blocks, h, r0, r1) for j, blocks, r0, r1 in steps]
        ready = products(*steps[0])
        for i, at in enumerate(steps):
            low_types = softmax_grad(*at, *ready)
            if i + 1 < len(steps):
                ready = products(*steps[i + 1])
            gradients(*at, *low_types)
            if after:
                after(at[0], at[1])

    own_low = ((6, 1, 0, 1), (6, 2, 1, 2))
    near_low = ((2, 4, 0, 1), (2, 4, 1, 2))
    far_low = ((0, 2, 0, 1), (1, 1, 1, 2))
    near_high = ((2, 4, 2, 3), (3, 3, 3, 4))
    own_high = ((6, 3, 2, 3), (6, 4, 3, 4))
    last_near = ((2, 1, 2, 3), (3, 1, 2, 4), (4, 2, 2, 4))

    def dq_copy(h, piece):
        columns = pl.ds(pl.multiple_of(h * HEAD, HEAD), HEAD)
        out_columns = pl.ds(pl.multiple_of(group * QCOLS + h * HEAD, HEAD), HEAD)
        return remote(
            dq_send.at[pl.ds(piece * TOK, TOK), columns], dq_out.at[:, out_columns],
            dq_send_sem.at[h, piece], dq_recv_sem.at[h, group], piece_device(piece),
        )

    def dq_local(h, piece):
        columns = pl.ds(pl.multiple_of(h * HEAD, HEAD), HEAD)
        out_columns = pl.ds(pl.multiple_of(group * QCOLS + h * HEAD, HEAD), HEAD)
        return pltpu.make_async_copy(
            dq_send.at[pl.ds(piece * TOK, TOK), columns], dq_out.at[:, out_columns], dq_recv_sem.at[h, group]
        )

    def finish_head(h, pieces):
        columns = pl.ds(pl.multiple_of(h * HEAD, HEAD), HEAD)
        rows = pl.ds(pieces[0] * TOK, HALF)
        dq_send[rows, columns] = (dq_t[h, :, rows].T * REST).astype(BF16)
        for piece in pieces:
            pl.when(mine != piece)(lambda: dq_copy(h, piece).start())
            pl.when(mine == piece)(lambda: dq_local(h, piece).start())

    def back_copies(j):
        rows = pl.ds(j * BLOCK, BLOCK)
        if j * BLOCK >= HALF:
            dsts, at, by = (dk_near, dv_near), pl.ds(j * BLOCK - HALF, BLOCK), -1
        else:
            dsts, at, by = (dk_far, dv_far), rows, -2
        return [
            remote(src.at[rows, :], dst.at[at, :], back_send.at[i, j], back_recv.at[i, j], span_device(by))
            for i, (src, dst) in enumerate(((dk_back, dsts[0]), (dv_back, dsts[1])))
        ]

    def send_back(j, blocks):
        rows = pl.ds(j * BLOCK, blocks * BLOCK)
        dk_back[rows, :] = (dk_acc[rows, :] * REST).astype(BF16)
        dv_back[rows, :] = (dv_acc[rows, :] * 2.0**SHIFT).astype(BF16)
        for at in range(j, j + blocks):
            start_all(back_copies(at))

    def low_head(h, carry):
        wait_head(h, low)
        pl.when((core == 1) & (h >= 1))(lambda: start_all(qe_copies(h - 1)))
        run(h, own_low)
        pl.when(has_prev & (h == 1))(lambda: wait_halo(range(PIECES), 1))
        pl.when(has_prev & (h >= 1))(lambda: run(h - 1, near_low))
        return carry

    lax.fori_loop(0, GROUP, low_head, 0)
    pl.when(core == 1)(lambda: start_all(qe_copies(GROUP - 1)))
    pl.when(has_prev)(lambda: run(GROUP - 1, near_low))
    pl.when(has_prev2)(lambda: wait_halo(high, 2))

    def far_head(h, carry):
        pl.when(has_prev2)(lambda: run(h, far_low))
        finish_head(h, low)
        return carry

    lax.fori_loop(0, GROUP, far_head, 0)
    pl.when(has_prev2)(lambda: send_back(0, 2))

    for piece in high:
        pl.when(mine != piece)(lambda: here(aux.at[piece], aux_recv.at[piece]).wait())

    def near_head(h, carry):
        wait_head(h, high)
        pl.when(has_prev)(lambda: run(h, near_high))
        return carry

    lax.fori_loop(0, GROUP - 1, near_head, 0)
    wait_head(GROUP - 1, high)

    pl.when(has_prev)(lambda: run(GROUP - 1, last_near, send_back))

    def high_head(h, carry):
        run(h, own_high)
        finish_head(h, high)
        return carry

    lax.fori_loop(0, GROUP, high_head, 0)

    def dkv_copies(piece):
        rows = pl.ds(piece * TOK, TOK)
        return [
            remote(
                src.at[rows, :], dst.at[:, cols(group, HEAD)],
                dkv_send_sem.at[i, piece], dkv_recv_sem.at[i, group], piece_device(piece),
            )
            for i, src, dst in ((0, dk_send, dk_out), (1, dv_send, dv_out))
        ]

    def dkv_local(piece):
        rows = pl.ds(piece * TOK, TOK)
        return [
            pltpu.make_async_copy(src.at[rows, :], dst.at[:, cols(group, HEAD)], dkv_recv_sem.at[i, group])
            for i, src, dst in ((0, dk_send, dk_out), (1, dv_send, dv_out))
        ]

    def finish_keys(b):
        rows = pl.ds(b * BLOCK, BLOCK)
        acc_rows = pl.ds(HALO + b * BLOCK, BLOCK)
        for i, acc, near, far, out, factor in (
            (0, dk_acc, dk_near, dk_far, dk_send, REST),
            (1, dv_acc, dv_near, dv_far, dv_send, 2.0**SHIFT),
        ):
            acc[acc_rows, :] *= factor

            def add_near():
                here(near.at[rows, :], back_recv.at[i, b + HALF // BLOCK]).wait()
                acc[acc_rows, :] += near[rows, :].astype(F32)

            def add_far():
                far_rows = pl.ds(b * BLOCK - HALF, BLOCK)
                here(far.at[far_rows, :], back_recv.at[i, b - HALF // BLOCK]).wait()
                acc[acc_rows, :] += far[far_rows, :].astype(F32)

            pl.when(has_next)(add_near)
            if b * BLOCK >= HALF:
                pl.when(has_next2)(add_far)
            out[rows, :] = acc[acc_rows, :].astype(BF16)
        for piece in (2 * b, 2 * b + 1):
            pl.when(mine != piece)(lambda: start_all(dkv_copies(piece)))
            pl.when(mine == piece)(lambda: start_all(dkv_local(piece)))

    for b in range(SPAN_BLOCKS):
        finish_keys(b)

    for g in range(PIECES):
        for h in range(GROUP):
            here(dq_out.at[:, pl.ds(g * QCOLS + h * HEAD, HEAD)], dq_recv_sem.at[h, g]).wait()
        here(dk_out.at[:, pl.ds(g * HEAD, HEAD)], dkv_recv_sem.at[0, g]).wait()
        here(dv_out.at[:, pl.ds(g * HEAD, HEAD)], dkv_recv_sem.at[1, g]).wait()
    def wait_sends(copies):
        for copy in copies:
            copy.wait_send()

    wait_sends(sends)
    for h in range(GROUP):
        wait_sends(qe_copies(h))

    for piece in range(PIECES):
        pl.when(has_next)(lambda: wait_sends(halo_copies(1, piece)))
        if piece >= Y:
            pl.when(has_next2)(lambda: wait_sends(halo_copies(2, piece)))
        pl.when(mine != piece)(lambda: wait_sends([dq_copy(h, piece) for h in range(GROUP)] + dkv_copies(piece)))
    for j in range(HALO_BLOCKS):
        pl.when(has_prev if j * BLOCK >= HALF else has_prev2)(lambda: wait_sends(back_copies(j)))


def store(*refs):
    sems = refs[-1]
    copies = [pltpu.make_async_copy(refs[i], refs[i + 3], sems.at[i]) for i in range(3)]
    for copy in copies:
        copy.start()
    for copy in copies:
        copy.wait()


def shards(n_span, query, key, value, out, output_gradient, log_sum_exp, segment_ids):
    hbm = pl.BlockSpec(memory_space=pltpu.HBM)
    dma = pltpu.SemaphoreType.DMA
    shape = jax.ShapeDtypeStruct
    window = HALO + SPAN
    args = (query, key, value, out, output_gradient, log_sum_exp.T, segment_ids.reshape(-1, TOK))
    args = [pltpu.with_memory_space_constraint(a, pltpu.HBM) for a in args]
    grads = pl.pallas_call(
        functools.partial(kernel, n_span),
        out_shape=[
            shape(query.shape, BF16),
            shape(key.shape, BF16),
            shape(value.shape, BF16),
        ],
        in_specs=[hbm] * 7,
        out_specs=[hbm] * 3,
        scratch_shapes=[
            pltpu.VMEM((TOK, PIECES * HEAD), BF16),
            pltpu.VMEM((TOK, PIECES * HEAD), BF16),
            pltpu.VMEM((TOK, PIECES * QCOLS), BF16),
            pltpu.VMEM((TOK, PIECES * QCOLS), BF16),
            pltpu.VMEM((PIECES * GROUP, TOK), F32),
            pltpu.VMEM((segment_ids.shape[0] // TOK, TOK), jnp.int32),
            pltpu.VMEM((PIECES, 2 * GROUP, TOK), F32),
            pltpu.VMEM((window, HEAD), BF16),
            pltpu.VMEM((window, HEAD), BF16),
            pltpu.VMEM((SPAN, QCOLS), BF16),
            pltpu.VMEM((SPAN, QCOLS), BF16),
            pltpu.VMEM((PIECES, 2 * GROUP, TOK), F32),
            pltpu.VMEM((window, TOK), jnp.int32),
            pltpu.VMEM((1, SPAN), jnp.int32),
            pltpu.VMEM((GROUP, HEAD, SPAN), F32),
            pltpu.VMEM((window, HEAD), F32),
            pltpu.VMEM((window, HEAD), F32),
            pltpu.VMEM((SPAN, QCOLS), BF16),
            pltpu.VMEM((SPAN, HEAD), BF16),
            pltpu.VMEM((SPAN, HEAD), BF16),
            pltpu.VMEM((HALO, HEAD), BF16),
            pltpu.VMEM((HALO, HEAD), BF16),
            pltpu.VMEM((SPAN, HEAD), BF16),
            pltpu.VMEM((SPAN, HEAD), BF16),
            pltpu.VMEM((HALF, HEAD), BF16),
            pltpu.VMEM((HALF, HEAD), BF16),
            dma((6,)),
            dma((2, PIECES)),
            dma((2, PIECES)),
            dma((PIECES,)),
            dma((PIECES,)),
            dma((2, GROUP, PIECES)),
            dma((2, GROUP, PIECES)),
            dma((2, PIECES + Y)),
            dma((2, PIECES + Y)),
            dma((2, HALO_BLOCKS)),
            dma((2, HALO_BLOCKS)),
            dma((GROUP, PIECES)),
            dma((GROUP, PIECES)),
            dma((2, PIECES)),
            dma((2, PIECES)),
        ],
        name="attention_backward",
        compiler_params=pltpu.CompilerParams(
            collective_id=0, has_side_effects=True, vmem_limit_bytes=40 * 2**20
        ),
    )(*args)
    return pl.pallas_call(
        store,
        out_shape=[shape(g.shape, BF16) for g in grads],
        in_specs=[pl.BlockSpec(memory_space=pltpu.VMEM)] * 3,
        out_specs=[hbm] * 3,
        scratch_shapes=[dma((3,))],
        name="store_gradients",
    )(*[pltpu.with_memory_space_constraint(g, pltpu.VMEM) for g in grads])


def solution(mesh):
    rows = P(("seq", "head"), None)
    return jax.shard_map(
        functools.partial(shards, mesh.shape["seq"] // 2),
        mesh=mesh,
        in_specs=(rows,) * 6 + (P(),),
        out_specs=(rows,) * 3,
        check_vma=False,
    )
```

```python
import functools
import math

import jax
import jax.numpy as jnp
from jax import lax
from jax.experimental import pallas as pl
from jax.experimental.pallas import tpu as pltpu
from jax.sharding import PartitionSpec as P

MESH = pl.DeviceIdType.MESH
BF16 = jnp.bfloat16
F32 = jnp.float32

HEAD = 128
TOK = 128
GROUP = 4
Y = 4
PIECES = 8
SPAN = PIECES * TOK
HALF = SPAN // 2
HALO = SPAN + HALF
BLOCK = 256
HALO_BLOCKS = HALO // BLOCK
SPAN_BLOCKS = SPAN // BLOCK
QCOLS = GROUP * HEAD

LOG2E = math.log2(math.e)
SCALE = 1.0 / math.sqrt(HEAD)
SHIFT = 4.0
REST = SCALE * 2.0**SHIFT
NT = (((1,), (1,)), ((), ()))
TN = (((0,), (0,)), ((), ()))


def kernel(
    n_span,
    q_hbm, k_hbm, v_hbm, o_hbm, e_hbm, lse_hbm, seg_hbm,
    dq_out, dk_out, dv_out,
    k_src, v_src, o_src, e_src, lse_ref, seg_ref, aux_src,
    k_all, v_all, q_all, e_all, aux, seg_k, seg_q,
    dq_t, dk_acc, dv_acc,
    dq_send, dk_send, dv_send, dk_back, dv_back, dk_near, dv_near, dk_far, dv_far,
    load_sem, kv_send, kv_recv, aux_send, aux_recv, qe_send, qe_recv,
    halo_send, halo_recv, back_send, back_recv,
    dq_send_sem, dq_recv_sem, dkv_send_sem, dkv_recv_sem,
):
    seq = lax.axis_index("seq")
    y = lax.axis_index("head")
    span = lax.div(seq, 2)
    core = lax.rem(seq, 2)
    mine = core * Y + y
    group = y * 2 + core

    def piece_device(piece):
        return (span * 2 + piece // Y, piece % Y)

    def span_device(by):
        return (seq + 2 * by, y)

    peers = []
    for dy in (1, 3, 0, 2):
        for dcore in (1, 0):
            if dy or dcore:
                py = lax.rem(y + dy, Y)
                pcore = lax.rem(core + dcore, 2)
                peers.append((dy * 2 + dcore, (span * 2 + pcore, py), py * 2 + pcore))

    has_prev, has_prev2 = span >= 1, span >= 2
    has_next, has_next2 = span < n_span - 1, span < n_span - 2

    def cols(g, width):
        return pl.ds(pl.multiple_of(g * width, width), width)

    my_rows = pl.ds(pl.multiple_of(mine * TOK, TOK), TOK)
    my_key_rows = pl.ds(pl.multiple_of(HALO + mine * TOK, TOK), TOK)
    loads = [
        pltpu.make_async_copy(src, dst, load_sem.at[i])
        for i, (src, dst) in enumerate(
            (
                (k_hbm, k_src), (v_hbm, v_src), (e_hbm, e_src), (o_hbm, o_src),
                (lse_hbm, lse_ref), (seg_hbm, seg_ref),
            )
        )
    ]
    own = [
        pltpu.make_async_copy(k_hbm.at[:, cols(group, HEAD)], k_all.at[my_key_rows, :], kv_recv.at[0, mine]),
        pltpu.make_async_copy(v_hbm.at[:, cols(group, HEAD)], v_all.at[my_key_rows, :], kv_recv.at[1, mine]),
    ]
    for h in range(GROUP):
        columns = pl.ds(pl.multiple_of(group * QCOLS + h * HEAD, HEAD), HEAD)
        for i, (src, dst) in enumerate(((q_hbm, q_all), (e_hbm, e_all))):
            own.append(
                pltpu.make_async_copy(
                    src.at[:, columns], dst.at[my_rows, pl.ds(h * HEAD, HEAD)], qe_recv.at[i, h, mine]
                )
            )
    for copy in loads + own:
        copy.start()

    barrier = pltpu.get_barrier_semaphore()

    def greet(device):
        pl.semaphore_signal(barrier, inc=1, device_id=device, device_id_type=MESH)

    for _, device, _ in peers:
        greet(device)
    pl.when(has_prev)(lambda: greet(span_device(-1)))
    pl.when(has_prev2)(lambda: greet(span_device(-2)))
    pl.when(has_next)(lambda: greet(span_device(1)))
    pl.when(has_next2)(lambda: greet(span_device(2)))
    neighbours = jnp.minimum(span, 2) + jnp.minimum(n_span - 1 - span, 2)
    pl.semaphore_wait(barrier, len(peers) + neighbours)

    def remote(src, dst, send, recv, device):
        return pltpu.make_async_remote_copy(
            src_ref=src, dst_ref=dst, send_sem=send, recv_sem=recv, device_id=device, device_id_type=MESH
        )

    sends = []
    loads[0].wait()
    loads[1].wait()
    for n, device, g in peers:
        for i, (src, dst) in enumerate(((k_src, k_all), (v_src, v_all))):
            sends.append(
                remote(src.at[:, cols(g, HEAD)], dst.at[my_key_rows, :], kv_send.at[i, n], kv_recv.at[i, mine], device)
            )
            sends[-1].start()

    def qe_copies(h):
        copies = []
        for n, device, g in peers:
            columns = pl.ds(pl.multiple_of(g * QCOLS + h * HEAD, HEAD), HEAD)
            at_columns = pl.ds(pl.multiple_of(h * HEAD, HEAD), HEAD)
            for i, (src, dst) in enumerate(((q_hbm, q_all), (e_src, e_all))):
                copies.append(
                    remote(
                        src.at[:, columns], dst.at[my_rows, at_columns],
                        qe_send.at[i, h, n], qe_recv.at[i, h, mine], device,
                    )
                )
        return copies

    def start_all(copies):
        for copy in copies:
            copy.start()

    loads[2].wait()
    pl.when(core == 0)(lambda: start_all(qe_copies(0)))

    loads[3].wait()
    loads[4].wait()
    lane = lax.broadcasted_iota(jnp.int32, (TOK, HEAD), 1)
    delta = jnp.zeros((TOK, HEAD), F32)
    for head in range(PIECES * GROUP):
        part = pl.ds(head * HEAD, HEAD)
        product = e_src[:, part].astype(F32) * o_src[:, part].astype(F32)
        delta = jnp.where(lane == head, jnp.sum(product, axis=1, keepdims=True), delta)
    delta = delta.T
    lse = lse_ref[...] * LOG2E + SHIFT
    for g in range(PIECES):
        aux_src[g, 0:GROUP, :] = lse[g * GROUP : (g + 1) * GROUP, :]
        aux_src[g, GROUP : 2 * GROUP, :] = delta[g * GROUP : (g + 1) * GROUP, :]
    for n, device, g in peers:
        sends.append(remote(aux_src.at[g], aux.at[mine], aux_send.at[n], aux_recv.at[mine], device))
        sends[-1].start()
    aux[mine] = aux_src[group]
    pl.when(core == 0)(lambda: [start_all(qe_copies(h)) for h in range(1, GROUP)] and None)

    def halo_copies(by, piece):
        rows = pl.ds(pl.multiple_of(HALO + piece * TOK, TOK), TOK)
        to = pl.ds(pl.multiple_of((HALF if by == 1 else -HALF) + piece * TOK, TOK), TOK)
        at = piece if by == 1 else piece + Y
        return [
            remote(ref.at[rows, :], ref.at[to, :], halo_send.at[i, at], halo_recv.at[i, at], span_device(by))
            for i, ref in enumerate((k_all, v_all))
        ]

    def here(ref, sem):
        return pltpu.make_async_copy(ref, ref, sem)

    for dy, dcore in ((0, 0), (0, 1), (1, 0), (3, 0), (1, 1), (3, 1), (2, 0), (2, 1)):
        piece = lax.rem(core + dcore, 2) * Y + lax.rem(y + dy, Y)
        rows = pl.ds(pl.multiple_of(HALO + piece * TOK, TOK), TOK)
        here(k_all.at[rows, :], kv_recv.at[0, piece]).wait()
        here(v_all.at[rows, :], kv_recv.at[1, piece]).wait()
        pl.when(has_next)(lambda: start_all(halo_copies(1, piece)))
    for piece in range(Y, PIECES):
        pl.when(has_next2)(lambda: start_all(halo_copies(2, piece)))

    loads[5].wait()
    first = span * PIECES - HALO // TOK
    for i in range((HALO + SPAN) // TOK):
        row = seg_ref[pl.ds(jnp.maximum(first + i, 0), 1), :]
        row = jnp.where(first + i < 0, -1, row)
        seg_k[pl.ds(i * TOK, TOK), :] = jnp.broadcast_to(row, (TOK, TOK)).T
        if i >= HALO // TOK:
            seg_q[:, pl.ds(i * TOK - HALO, TOK)] = row

    dk_acc[...] = jnp.zeros_like(dk_acc)
    dv_acc[...] = jnp.zeros_like(dv_acc)
    dq_t[...] = jnp.zeros_like(dq_t)

    for piece in range(Y):
        pl.when(mine != piece)(lambda: here(aux.at[piece], aux_recv.at[piece]).wait())

    def where(j, blocks, h, r0, r1):
        keys = pl.ds(j * BLOCK, blocks * BLOCK)
        rows = pl.ds(r0 * BLOCK, (r1 - r0) * BLOCK)
        return keys, rows, pl.ds(pl.multiple_of(h * HEAD, HEAD), HEAD)

    def products(j, blocks, h, r0, r1):
        keys, rows, columns = where(j, blocks, h, r0, r1)
        scores = lax.dot_general(k_all[keys, :], q_all[rows, columns], NT, preferred_element_type=F32)
        dprobs = lax.dot_general(v_all[keys, :], e_all[rows, columns], NT, preferred_element_type=F32)
        return scores, dprobs

    def softmax_grad(j, blocks, h, r0, r1, scores, dprobs):
        keys, rows, _ = where(j, blocks, h, r0, r1)
        height, width = blocks * BLOCK, (r1 - r0) * BLOCK
        pieces = range(r0 * BLOCK // TOK, r1 * BLOCK // TOK)
        lse = jnp.concatenate([aux[p, pl.ds(h, 1), :] for p in pieces], axis=1)
        delta = jnp.concatenate([aux[p, pl.ds(h + GROUP, 1), :] for p in pieces], axis=1)
        doc = jnp.concatenate([seg_k[keys, :]] * (width // TOK), axis=1)
        allowed = doc == seg_q[:, rows]
        if j + blocks - 1 - HALO_BLOCKS >= r0:
            key_at = lax.broadcasted_iota(jnp.int32, (height, width), 0) + (j - HALO_BLOCKS) * BLOCK
            query_at = lax.broadcasted_iota(jnp.int32, (height, width), 1) + r0 * BLOCK
            allowed = allowed & (key_at <= query_at)
        probs = jnp.exp2(jnp.where(allowed, scores * (SCALE * LOG2E) - lse, -jnp.inf))
        return probs.astype(BF16), (probs * (dprobs - delta)).astype(BF16)

    def gradients(j, blocks, h, r0, r1, probs, dscores):
        keys, rows, columns = where(j, blocks, h, r0, r1)
        dv_acc[keys, :] += jnp.dot(probs, e_all[rows, columns], preferred_element_type=F32)
        dk_acc[keys, :] += jnp.dot(dscores, q_all[rows, columns], preferred_element_type=F32)
        dq_t[h, :, rows] += lax.dot_general(k_all[keys, :], dscores, TN, preferred_element_type=F32)

    def wait_head(h, pieces):
        columns = pl.ds(pl.multiple_of(h * HEAD, HEAD), HEAD)
        for piece in pieces:
            rows = pl.ds(piece * TOK, TOK)
            here(q_all.at[rows, columns], qe_recv.at[0, h, piece]).wait()
            here(e_all.at[rows, columns], qe_recv.at[1, h, piece]).wait()

    def wait_halo(pieces, by):
        for piece in pieces:
            at = piece if by == 1 else piece + Y
            rows = pl.ds((HALF if by == 1 else -HALF) + piece * TOK, TOK)
            here(k_all.at[rows, :], halo_recv.at[0, at]).wait()
            here(v_all.at[rows, :], halo_recv.at[1, at]).wait()

    low, high = range(Y), range(Y, PIECES)

    def run(h, steps, after=None):
        steps = [(j, blocks, h, r0, r1) for j, blocks, r0, r1 in steps]
        ready = products(*steps[0])
        for i, at in enumerate(steps):
            low_types = softmax_grad(*at, *ready)
            if i + 1 < len(steps):
                ready = products(*steps[i + 1])
            gradients(*at, *low_types)
            if after:
                after(at[0], at[1])

    own_low = ((6, 1, 0, 1), (6, 2, 1, 2))
    near_low = ((2, 4, 0, 1), (2, 4, 1, 2))
    far_low = ((0, 2, 0, 1), (1, 1, 1, 2))
    near_high = ((2, 4, 2, 3), (3, 3, 3, 4))
    own_high = ((6, 3, 2, 3), (6, 4, 3, 4))
    last_near = ((2, 1, 2, 3), (3, 1, 2, 4), (4, 2, 2, 4))

    def dq_copy(h, piece):
        columns = pl.ds(pl.multiple_of(h * HEAD, HEAD), HEAD)
        out_columns = pl.ds(pl.multiple_of(group * QCOLS + h * HEAD, HEAD), HEAD)
        return remote(
            dq_send.at[pl.ds(piece * TOK, TOK), columns], dq_out.at[:, out_columns],
            dq_send_sem.at[h, piece], dq_recv_sem.at[h, group], piece_device(piece),
        )

    def dq_local(h, piece):
        columns = pl.ds(pl.multiple_of(h * HEAD, HEAD), HEAD)
        out_columns = pl.ds(pl.multiple_of(group * QCOLS + h * HEAD, HEAD), HEAD)
        return pltpu.make_async_copy(
            dq_send.at[pl.ds(piece * TOK, TOK), columns], dq_out.at[:, out_columns], dq_recv_sem.at[h, group]
        )

    def finish_head(h, pieces):
        columns = pl.ds(pl.multiple_of(h * HEAD, HEAD), HEAD)
        rows = pl.ds(pieces[0] * TOK, HALF)
        dq_send[rows, columns] = (dq_t[h, :, rows].T * REST).astype(BF16)
        for piece in pieces:
            pl.when(mine != piece)(lambda: dq_copy(h, piece).start())
            pl.when(mine == piece)(lambda: dq_local(h, piece).start())

    def back_copies(j):
        rows = pl.ds(j * BLOCK, BLOCK)
        if j * BLOCK >= HALF:
            dsts, at, by = (dk_near, dv_near), pl.ds(j * BLOCK - HALF, BLOCK), -1
        else:
            dsts, at, by = (dk_far, dv_far), rows, -2
        return [
            remote(src.at[rows, :], dst.at[at, :], back_send.at[i, j], back_recv.at[i, j], span_device(by))
            for i, (src, dst) in enumerate(((dk_back, dsts[0]), (dv_back, dsts[1])))
        ]

    def send_back(j, blocks):
        rows = pl.ds(j * BLOCK, blocks * BLOCK)
        dk_back[rows, :] = (dk_acc[rows, :] * REST).astype(BF16)
        dv_back[rows, :] = (dv_acc[rows, :] * 2.0**SHIFT).astype(BF16)
        for at in range(j, j + blocks):
            start_all(back_copies(at))

    def low_head(h, carry):
        wait_head(h, low)
        pl.when((core == 1) & (h >= 1))(lambda: start_all(qe_copies(h - 1)))
        run(h, own_low)
        pl.when(has_prev & (h == 1))(lambda: wait_halo(range(PIECES), 1))
        pl.when(has_prev & (h >= 1))(lambda: run(h - 1, near_low))
        return carry

    lax.fori_loop(0, GROUP, low_head, 0)
    pl.when(core == 1)(lambda: start_all(qe_copies(GROUP - 1)))
    pl.when(has_prev)(lambda: run(GROUP - 1, near_low))
    pl.when(has_prev2)(lambda: wait_halo(high, 2))

    def far_head(h, carry):
        pl.when(has_prev2)(lambda: run(h, far_low))
        finish_head(h, low)
        return carry

    lax.fori_loop(0, GROUP, far_head, 0)
    pl.when(has_prev2)(lambda: send_back(0, 2))

    for piece in high:
        pl.when(mine != piece)(lambda: here(aux.at[piece], aux_recv.at[piece]).wait())

    def near_head(h, carry):
        wait_head(h, high)
        pl.when(has_prev)(lambda: run(h, near_high))
        return carry

    lax.fori_loop(0, GROUP - 1, near_head, 0)
    wait_head(GROUP - 1, high)

    pl.when(has_prev)(lambda: run(GROUP - 1, last_near, send_back))

    def high_head(h, carry):
        run(h, own_high)
        finish_head(h, high)
        return carry

    lax.fori_loop(0, GROUP, high_head, 0)

    def dkv_copies(piece):
        rows = pl.ds(piece * TOK, TOK)
        return [
            remote(
                src.at[rows, :], dst.at[:, cols(group, HEAD)],
                dkv_send_sem.at[i, piece], dkv_recv_sem.at[i, group], piece_device(piece),
            )
            for i, src, dst in ((0, dk_send, dk_out), (1, dv_send, dv_out))
        ]

    def dkv_local(piece):
        rows = pl.ds(piece * TOK, TOK)
        return [
            pltpu.make_async_copy(src.at[rows, :], dst.at[:, cols(group, HEAD)], dkv_recv_sem.at[i, group])
            for i, src, dst in ((0, dk_send, dk_out), (1, dv_send, dv_out))
        ]

    def finish_keys(b):
        rows = pl.ds(b * BLOCK, BLOCK)
        acc_rows = pl.ds(HALO + b * BLOCK, BLOCK)
        for i, acc, near, far, out, factor in (
            (0, dk_acc, dk_near, dk_far, dk_send, REST),
            (1, dv_acc, dv_near, dv_far, dv_send, 2.0**SHIFT),
        ):
            acc[acc_rows, :] *= factor

            def add_near():
                here(near.at[rows, :], back_recv.at[i, b + HALF // BLOCK]).wait()
                acc[acc_rows, :] += near[rows, :].astype(F32)

            def add_far():
                far_rows = pl.ds(b * BLOCK - HALF, BLOCK)
                here(far.at[far_rows, :], back_recv.at[i, b - HALF // BLOCK]).wait()
                acc[acc_rows, :] += far[far_rows, :].astype(F32)

            pl.when(has_next)(add_near)
            if b * BLOCK >= HALF:
                pl.when(has_next2)(add_far)
            out[rows, :] = acc[acc_rows, :].astype(BF16)
        for piece in (2 * b, 2 * b + 1):
            pl.when(mine != piece)(lambda: start_all(dkv_copies(piece)))
            pl.when(mine == piece)(lambda: start_all(dkv_local(piece)))

    for b in range(SPAN_BLOCKS):
        finish_keys(b)

    for g in range(PIECES):
        for h in range(GROUP):
            here(dq_out.at[:, pl.ds(g * QCOLS + h * HEAD, HEAD)], dq_recv_sem.at[h, g]).wait()
        here(dk_out.at[:, pl.ds(g * HEAD, HEAD)], dkv_recv_sem.at[0, g]).wait()
        here(dv_out.at[:, pl.ds(g * HEAD, HEAD)], dkv_recv_sem.at[1, g]).wait()
    def wait_sends(copies):
        for copy in copies:
            copy.wait_send()

    wait_sends(sends)
    for h in range(GROUP):
        wait_sends(qe_copies(h))

    for piece in range(PIECES):
        pl.when(has_next)(lambda: wait_sends(halo_copies(1, piece)))
        if piece >= Y:
            pl.when(has_next2)(lambda: wait_sends(halo_copies(2, piece)))
        pl.when(mine != piece)(lambda: wait_sends([dq_copy(h, piece) for h in range(GROUP)] + dkv_copies(piece)))
    for j in range(HALO_BLOCKS):
        pl.when(has_prev if j * BLOCK >= HALF else has_prev2)(lambda: wait_sends(back_copies(j)))


def store(*refs):
    sems = refs[-1]
    copies = [pltpu.make_async_copy(refs[i], refs[i + 3], sems.at[i]) for i in range(3)]
    for copy in copies:
        copy.start()
    for copy in copies:
        copy.wait()


def shards(n_span, query, key, value, out, output_gradient, log_sum_exp, segment_ids):
    hbm = pl.BlockSpec(memory_space=pltpu.HBM)
    dma = pltpu.SemaphoreType.DMA
    shape = jax.ShapeDtypeStruct
    window = HALO + SPAN
    args = (query, key, value, out, output_gradient, log_sum_exp.T, segment_ids.reshape(-1, TOK))
    args = [pltpu.with_memory_space_constraint(a, pltpu.HBM) for a in args]
    grads = pl.pallas_call(
        functools.partial(kernel, n_span),
        out_shape=[
            shape(query.shape, BF16),
            shape(key.shape, BF16),
            shape(value.shape, BF16),
        ],
        in_specs=[hbm] * 7,
        out_specs=[hbm] * 3,
        scratch_shapes=[
            pltpu.VMEM((TOK, PIECES * HEAD), BF16),
            pltpu.VMEM((TOK, PIECES * HEAD), BF16),
            pltpu.VMEM((TOK, PIECES * QCOLS), BF16),
            pltpu.VMEM((TOK, PIECES * QCOLS), BF16),
            pltpu.VMEM((PIECES * GROUP, TOK), F32),
            pltpu.VMEM((segment_ids.shape[0] // TOK, TOK), jnp.int32),
            pltpu.VMEM((PIECES, 2 * GROUP, TOK), F32),
            pltpu.VMEM((window, HEAD), BF16),
            pltpu.VMEM((window, HEAD), BF16),
            pltpu.VMEM((SPAN, QCOLS), BF16),
            pltpu.VMEM((SPAN, QCOLS), BF16),
            pltpu.VMEM((PIECES, 2 * GROUP, TOK), F32),
            pltpu.VMEM((window, TOK), jnp.int32),
            pltpu.VMEM((1, SPAN), jnp.int32),
            pltpu.VMEM((GROUP, HEAD, SPAN), F32),
            pltpu.VMEM((window, HEAD), F32),
            pltpu.VMEM((window, HEAD), F32),
            pltpu.VMEM((SPAN, QCOLS), BF16),
            pltpu.VMEM((SPAN, HEAD), BF16),
            pltpu.VMEM((SPAN, HEAD), BF16),
            pltpu.VMEM((HALO, HEAD), BF16),
            pltpu.VMEM((HALO, HEAD), BF16),
            pltpu.VMEM((SPAN, HEAD), BF16),
            pltpu.VMEM((SPAN, HEAD), BF16),
            pltpu.VMEM((HALF, HEAD), BF16),
            pltpu.VMEM((HALF, HEAD), BF16),
            dma((6,)),
            dma((2, PIECES)),
            dma((2, PIECES)),
            dma((PIECES,)),
            dma((PIECES,)),
            dma((2, GROUP, PIECES)),
            dma((2, GROUP, PIECES)),
            dma((2, PIECES + Y)),
            dma((2, PIECES + Y)),
            dma((2, HALO_BLOCKS)),
            dma((2, HALO_BLOCKS)),
            dma((GROUP, PIECES)),
            dma((GROUP, PIECES)),
            dma((2, PIECES)),
            dma((2, PIECES)),
        ],
        name="attention_backward",
        compiler_params=pltpu.CompilerParams(
            collective_id=0, has_side_effects=True, vmem_limit_bytes=40 * 2**20
        ),
    )(*args)
    return pl.pallas_call(
        store,
        out_shape=[shape(g.shape, BF16) for g in grads],
        in_specs=[pl.BlockSpec(memory_space=pltpu.VMEM)] * 3,
        out_specs=[hbm] * 3,
        scratch_shapes=[dma((3,))],
        name="store_gradients",
    )(*[pltpu.with_memory_space_constraint(g, pltpu.VMEM) for g in grads])


def solution(mesh):
    rows = P(("seq", "head"), None)
    return jax.shard_map(
        functools.partial(shards, mesh.shape["seq"] // 2),
        mesh=mesh,
        in_specs=(rows,) * 6 + (P(),),
        out_specs=(rows,) * 3,
        check_vma=False,
    )
```

```python
import functools
import math

import jax
import jax.numpy as jnp
from jax import lax
from jax.experimental import pallas as pl
from jax.experimental.pallas import tpu as pltpu
from jax.sharding import PartitionSpec as P

MESH = pl.DeviceIdType.MESH
BF16 = jnp.bfloat16
F32 = jnp.float32

HEAD = 128
TOK = 128
GROUP = 4
Y = 4
PIECES = 8
SPAN = PIECES * TOK
HALF = SPAN // 2
HALO = SPAN + HALF
BLOCK = 256
HALO_BLOCKS = HALO // BLOCK
SPAN_BLOCKS = SPAN // BLOCK
QCOLS = GROUP * HEAD

LOG2E = math.log2(math.e)
SCALE = 1.0 / math.sqrt(HEAD)
SHIFT = 4.0
REST = SCALE * 2.0**SHIFT
NT = (((1,), (1,)), ((), ()))
TN = (((0,), (0,)), ((), ()))


def kernel(
    n_span,
    q_hbm, k_hbm, v_hbm, o_hbm, e_hbm, lse_hbm, seg_hbm,
    dq_out, dk_out, dv_out,
    k_src, v_src, o_src, e_src, q_src, lse_ref, seg_ref, aux_src,
    k_all, v_all, q_all, e_all, aux, seg_k, seg_q,
    dq_t, dk_acc, dv_acc,
    dq_send, dk_send, dv_send, dk_back, dv_back, dk_near, dv_near, dk_far, dv_far,
    load_sem, kv_send, kv_recv, aux_send, aux_recv, qe_send, qe_recv,
    halo_send, halo_recv, back_send, back_recv,
    dq_send_sem, dq_recv_sem, dkv_send_sem, dkv_recv_sem,
):
    seq = lax.axis_index("seq")
    y = lax.axis_index("head")
    span = lax.div(seq, 2)
    core = lax.rem(seq, 2)
    mine = core * Y + y
    group = y * 2 + core

    def piece_device(piece):
        return (span * 2 + piece // Y, piece % Y)

    def span_device(by):
        return (seq + 2 * by, y)

    peers = []
    for dy in (1, 3, 0, 2):
        for dcore in (1, 0):
            if dy or dcore:
                py = lax.rem(y + dy, Y)
                pcore = lax.rem(core + dcore, 2)
                peers.append((dy * 2 + dcore, (span * 2 + pcore, py), py * 2 + pcore))

    has_prev, has_prev2 = span >= 1, span >= 2
    has_next, has_next2 = span < n_span - 1, span < n_span - 2

    def cols(g, width):
        return pl.ds(pl.multiple_of(g * width, width), width)

    my_rows = pl.ds(pl.multiple_of(mine * TOK, TOK), TOK)
    my_key_rows = pl.ds(pl.multiple_of(HALO + mine * TOK, TOK), TOK)
    loads = [
        pltpu.make_async_copy(src, dst, load_sem.at[i])
        for i, (src, dst) in enumerate(
            (
                (k_hbm, k_src), (v_hbm, v_src), (e_hbm, e_src), (o_hbm, o_src),
                (lse_hbm, lse_ref), (seg_hbm, seg_ref), (q_hbm, q_src),
            )
        )
    ]
    own = [
        pltpu.make_async_copy(k_hbm.at[:, cols(group, HEAD)], k_all.at[my_key_rows, :], kv_recv.at[0, mine]),
        pltpu.make_async_copy(v_hbm.at[:, cols(group, HEAD)], v_all.at[my_key_rows, :], kv_recv.at[1, mine]),
    ]
    for h in range(GROUP):
        columns = pl.ds(pl.multiple_of(group * QCOLS + h * HEAD, HEAD), HEAD)
        for i, (src, dst) in enumerate(((q_hbm, q_all), (e_hbm, e_all))):
            own.append(
                pltpu.make_async_copy(
                    src.at[:, columns], dst.at[my_rows, pl.ds(h * HEAD, HEAD)], qe_recv.at[i, h, mine]
                )
            )
    for copy in loads + own:
        copy.start()

    barrier = pltpu.get_barrier_semaphore()

    def greet(device):
        pl.semaphore_signal(barrier, inc=1, device_id=device, device_id_type=MESH)

    for _, device, _ in peers:
        greet(device)
    pl.when(has_prev)(lambda: greet(span_device(-1)))
    pl.when(has_prev2)(lambda: greet(span_device(-2)))
    pl.when(has_next)(lambda: greet(span_device(1)))
    pl.when(has_next2)(lambda: greet(span_device(2)))
    neighbours = jnp.minimum(span, 2) + jnp.minimum(n_span - 1 - span, 2)
    pl.semaphore_wait(barrier, len(peers) + neighbours)

    def remote(src, dst, send, recv, device):
        return pltpu.make_async_remote_copy(
            src_ref=src, dst_ref=dst, send_sem=send, recv_sem=recv, device_id=device, device_id_type=MESH
        )

    sends = []
    loads[0].wait()
    loads[1].wait()
    for n, device, g in peers:
        for i, (src, dst) in enumerate(((k_src, k_all), (v_src, v_all))):
            sends.append(
                remote(src.at[:, cols(g, HEAD)], dst.at[my_key_rows, :], kv_send.at[i, n], kv_recv.at[i, mine], device)
            )
            sends[-1].start()

    def qe_copies(h):
        copies = []
        for n, device, g in peers:
            columns = pl.ds(pl.multiple_of(g * QCOLS + h * HEAD, HEAD), HEAD)
            at_columns = pl.ds(pl.multiple_of(h * HEAD, HEAD), HEAD)
            for i, (src, dst) in enumerate(((q_src, q_all), (e_src, e_all))):
                copies.append(
                    remote(
                        src.at[:, columns], dst.at[my_rows, at_columns],
                        qe_send.at[i, h, n], qe_recv.at[i, h, mine], device,
                    )
                )
        return copies

    def start_all(copies):
        for copy in copies:
            copy.start()

    loads[2].wait()
    loads[6].wait()
    pl.when(core == 0)(lambda: start_all(qe_copies(0)))

    loads[3].wait()
    loads[4].wait()
    lane = lax.broadcasted_iota(jnp.int32, (TOK, HEAD), 1)
    delta = jnp.zeros((TOK, HEAD), F32)
    for head in range(PIECES * GROUP):
        part = pl.ds(head * HEAD, HEAD)
        product = e_src[:, part].astype(F32) * o_src[:, part].astype(F32)
        delta = jnp.where(lane == head, jnp.sum(product, axis=1, keepdims=True), delta)
    delta = delta.T
    lse = lse_ref[...] * LOG2E + SHIFT
    for g in range(PIECES):
        aux_src[g, 0:GROUP, :] = lse[g * GROUP : (g + 1) * GROUP, :]
        aux_src[g, GROUP : 2 * GROUP, :] = delta[g * GROUP : (g + 1) * GROUP, :]
    for n, device, g in peers:
        sends.append(remote(aux_src.at[g], aux.at[mine], aux_send.at[n], aux_recv.at[mine], device))
        sends[-1].start()
    aux[mine] = aux_src[group]
    pl.when(core == 0)(lambda: [start_all(qe_copies(h)) for h in range(1, GROUP)] and None)

    def halo_copies(by, piece):
        rows = pl.ds(pl.multiple_of(HALO + piece * TOK, TOK), TOK)
        to = pl.ds(pl.multiple_of((HALF if by == 1 else -HALF) + piece * TOK, TOK), TOK)
        at = piece if by == 1 else piece + Y
        return [
            remote(ref.at[rows, :], ref.at[to, :], halo_send.at[i, at], halo_recv.at[i, at], span_device(by))
            for i, ref in enumerate((k_all, v_all))
        ]

    def here(ref, sem):
        return pltpu.make_async_copy(ref, ref, sem)

    for dy, dcore in ((0, 0), (0, 1), (1, 1), (3, 1), (1, 0), (3, 0), (2, 1), (2, 0)):
        piece = lax.rem(core + dcore, 2) * Y + lax.rem(y + dy, Y)
        rows = pl.ds(pl.multiple_of(HALO + piece * TOK, TOK), TOK)
        here(k_all.at[rows, :], kv_recv.at[0, piece]).wait()
        here(v_all.at[rows, :], kv_recv.at[1, piece]).wait()
        pl.when(has_next)(lambda: start_all(halo_copies(1, piece)))
    for piece in range(Y, PIECES):
        pl.when(has_next2)(lambda: start_all(halo_copies(2, piece)))

    loads[5].wait()
    first = span * PIECES - HALO // TOK
    for i in range((HALO + SPAN) // TOK):
        row = seg_ref[pl.ds(jnp.maximum(first + i, 0), 1), :]
        row = jnp.where(first + i < 0, -1, row)
        seg_k[pl.ds(i * TOK, TOK), :] = jnp.broadcast_to(row, (TOK, TOK)).T
        if i >= HALO // TOK:
            seg_q[:, pl.ds(i * TOK - HALO, TOK)] = row

    dk_acc[...] = jnp.zeros_like(dk_acc)
    dv_acc[...] = jnp.zeros_like(dv_acc)
    dq_t[...] = jnp.zeros_like(dq_t)

    for piece in range(Y):
        pl.when(mine != piece)(lambda: here(aux.at[piece], aux_recv.at[piece]).wait())

    def where(j, blocks, h, r0, r1):
        keys = pl.ds(j * BLOCK, blocks * BLOCK)
        rows = pl.ds(r0 * BLOCK, (r1 - r0) * BLOCK)
        return keys, rows, pl.ds(pl.multiple_of(h * HEAD, HEAD), HEAD)

    def products(j, blocks, h, r0, r1):
        keys, rows, columns = where(j, blocks, h, r0, r1)
        scores = lax.dot_general(k_all[keys, :], q_all[rows, columns], NT, preferred_element_type=F32)
        dprobs = lax.dot_general(v_all[keys, :], e_all[rows, columns], NT, preferred_element_type=F32)
        return scores, dprobs

    def softmax_grad(j, blocks, h, r0, r1, scores, dprobs):
        keys, rows, _ = where(j, blocks, h, r0, r1)
        height, width = blocks * BLOCK, (r1 - r0) * BLOCK
        pieces = range(r0 * BLOCK // TOK, r1 * BLOCK // TOK)
        lse = jnp.concatenate([aux[p, pl.ds(h, 1), :] for p in pieces], axis=1)
        delta = jnp.concatenate([aux[p, pl.ds(h + GROUP, 1), :] for p in pieces], axis=1)
        doc = jnp.concatenate([seg_k[keys, :]] * (width // TOK), axis=1)
        allowed = doc == seg_q[:, rows]
        if j + blocks - 1 - HALO_BLOCKS >= r0:
            key_at = lax.broadcasted_iota(jnp.int32, (height, width), 0) + (j - HALO_BLOCKS) * BLOCK
            query_at = lax.broadcasted_iota(jnp.int32, (height, width), 1) + r0 * BLOCK
            allowed = allowed & (key_at <= query_at)
        probs = jnp.exp2(jnp.where(allowed, scores * (SCALE * LOG2E) - lse, -jnp.inf))
        return probs.astype(BF16), (probs * (dprobs - delta)).astype(BF16)

    def gradients(j, blocks, h, r0, r1, probs, dscores):
        keys, rows, columns = where(j, blocks, h, r0, r1)
        dv_acc[keys, :] += jnp.dot(probs, e_all[rows, columns], preferred_element_type=F32)
        dk_acc[keys, :] += jnp.dot(dscores, q_all[rows, columns], preferred_element_type=F32)
        dq_t[h, :, rows] += lax.dot_general(k_all[keys, :], dscores, TN, preferred_element_type=F32)

    def wait_head(h, pieces):
        columns = pl.ds(pl.multiple_of(h * HEAD, HEAD), HEAD)
        for piece in pieces:
            rows = pl.ds(piece * TOK, TOK)
            here(q_all.at[rows, columns], qe_recv.at[0, h, piece]).wait()
            here(e_all.at[rows, columns], qe_recv.at[1, h, piece]).wait()

    def wait_halo(pieces, by):
        for piece in pieces:
            at = piece if by == 1 else piece + Y
            rows = pl.ds((HALF if by == 1 else -HALF) + piece * TOK, TOK)
            here(k_all.at[rows, :], halo_recv.at[0, at]).wait()
            here(v_all.at[rows, :], halo_recv.at[1, at]).wait()

    low, high = range(Y), range(Y, PIECES)

    def run(h, steps, after=None):
        steps = [(j, blocks, h, r0, r1) for j, blocks, r0, r1 in steps]
        ready = products(*steps[0])
        for i, at in enumerate(steps):
            low_types = softmax_grad(*at, *ready)
            if i + 1 < len(steps):
                ready = products(*steps[i + 1])
            gradients(*at, *low_types)
            if after:
                after(at[0], at[1])

    own_low = ((6, 1, 0, 1), (6, 2, 1, 2))
    near_low = ((2, 4, 0, 1), (2, 4, 1, 2))
    far_low = ((0, 2, 0, 1), (1, 1, 1, 2))
    near_high = ((2, 4, 2, 3), (3, 3, 3, 4))
    own_high = ((6, 3, 2, 3), (6, 4, 3, 4))
    last_near = ((2, 1, 2, 3), (3, 1, 2, 4), (4, 2, 2, 4))

    def dq_copy(h, piece):
        columns = pl.ds(pl.multiple_of(h * HEAD, HEAD), HEAD)
        out_columns = pl.ds(pl.multiple_of(group * QCOLS + h * HEAD, HEAD), HEAD)
        return remote(
            dq_send.at[pl.ds(piece * TOK, TOK), columns], dq_out.at[:, out_columns],
            dq_send_sem.at[h, piece], dq_recv_sem.at[h, group], piece_device(piece),
        )

    def dq_local(h, piece):
        columns = pl.ds(pl.multiple_of(h * HEAD, HEAD), HEAD)
        out_columns = pl.ds(pl.multiple_of(group * QCOLS + h * HEAD, HEAD), HEAD)
        return pltpu.make_async_copy(
            dq_send.at[pl.ds(piece * TOK, TOK), columns], dq_out.at[:, out_columns], dq_recv_sem.at[h, group]
        )

    def finish_head(h, pieces):
        columns = pl.ds(pl.multiple_of(h * HEAD, HEAD), HEAD)
        rows = pl.ds(pieces[0] * TOK, HALF)
        dq_send[rows, columns] = (dq_t[h, :, rows].T * REST).astype(BF16)
        for piece in pieces:
            pl.when(mine != piece)(lambda: dq_copy(h, piece).start())
            pl.when(mine == piece)(lambda: dq_local(h, piece).start())

    def back_copies(j):
        rows = pl.ds(j * BLOCK, BLOCK)
        if j * BLOCK >= HALF:
            dsts, at, by = (dk_near, dv_near), pl.ds(j * BLOCK - HALF, BLOCK), -1
        else:
            dsts, at, by = (dk_far, dv_far), rows, -2
        return [
            remote(src.at[rows, :], dst.at[at, :], back_send.at[i, j], back_recv.at[i, j], span_device(by))
            for i, (src, dst) in enumerate(((dk_back, dsts[0]), (dv_back, dsts[1])))
        ]

    def send_back(j, blocks):
        rows = pl.ds(j * BLOCK, blocks * BLOCK)
        dk_back[rows, :] = (dk_acc[rows, :] * REST).astype(BF16)
        dv_back[rows, :] = (dv_acc[rows, :] * 2.0**SHIFT).astype(BF16)
        for at in range(j, j + blocks):
            start_all(back_copies(at))

    def low_head(h, carry):
        wait_head(h, low)
        pl.when((core == 1) & (h >= 1))(lambda: start_all(qe_copies(h - 1)))
        run(h, own_low)
        pl.when(has_prev & (h == 1))(lambda: wait_halo(range(PIECES), 1))
        pl.when(has_prev & (h >= 1))(lambda: run(h - 1, near_low))
        return carry

    lax.fori_loop(0, GROUP, low_head, 0)
    pl.when(core == 1)(lambda: start_all(qe_copies(GROUP - 1)))
    pl.when(has_prev)(lambda: run(GROUP - 1, near_low))
    pl.when(has_prev2)(lambda: wait_halo(high, 2))

    def far_head(h, carry):
        pl.when(has_prev2)(lambda: run(h, far_low))
        finish_head(h, low)
        return carry

    lax.fori_loop(0, GROUP, far_head, 0)
    pl.when(has_prev2)(lambda: send_back(0, 2))

    for piece in high:
        pl.when(mine != piece)(lambda: here(aux.at[piece], aux_recv.at[piece]).wait())

    def near_head(h, carry):
        wait_head(h, high)
        pl.when(has_prev)(lambda: run(h, near_high))
        return carry

    lax.fori_loop(0, GROUP - 1, near_head, 0)
    wait_head(GROUP - 1, high)

    pl.when(has_prev)(lambda: run(GROUP - 1, last_near, send_back))

    def high_head(h, carry):
        run(h, own_high)
        finish_head(h, high)
        return carry

    lax.fori_loop(0, GROUP, high_head, 0)

    def dkv_copies(piece):
        rows = pl.ds(piece * TOK, TOK)
        return [
            remote(
                src.at[rows, :], dst.at[:, cols(group, HEAD)],
                dkv_send_sem.at[i, piece], dkv_recv_sem.at[i, group], piece_device(piece),
            )
            for i, src, dst in ((0, dk_send, dk_out), (1, dv_send, dv_out))
        ]

    def dkv_local(piece):
        rows = pl.ds(piece * TOK, TOK)
        return [
            pltpu.make_async_copy(src.at[rows, :], dst.at[:, cols(group, HEAD)], dkv_recv_sem.at[i, group])
            for i, src, dst in ((0, dk_send, dk_out), (1, dv_send, dv_out))
        ]

    def finish_keys(b):
        rows = pl.ds(b * BLOCK, BLOCK)
        acc_rows = pl.ds(HALO + b * BLOCK, BLOCK)
        for i, acc, near, far, out, factor in (
            (0, dk_acc, dk_near, dk_far, dk_send, REST),
            (1, dv_acc, dv_near, dv_far, dv_send, 2.0**SHIFT),
        ):
            acc[acc_rows, :] *= factor

            def add_near():
                here(near.at[rows, :], back_recv.at[i, b + HALF // BLOCK]).wait()
                acc[acc_rows, :] += near[rows, :].astype(F32)

            def add_far():
                far_rows = pl.ds(b * BLOCK - HALF, BLOCK)
                here(far.at[far_rows, :], back_recv.at[i, b - HALF // BLOCK]).wait()
                acc[acc_rows, :] += far[far_rows, :].astype(F32)

            pl.when(has_next)(add_near)
            if b * BLOCK >= HALF:
                pl.when(has_next2)(add_far)
            out[rows, :] = acc[acc_rows, :].astype(BF16)
        for piece in (2 * b, 2 * b + 1):
            pl.when(mine != piece)(lambda: start_all(dkv_copies(piece)))
            pl.when(mine == piece)(lambda: start_all(dkv_local(piece)))

    for b in range(SPAN_BLOCKS):
        finish_keys(b)

    for g in range(PIECES):
        for h in range(GROUP):
            here(dq_out.at[:, pl.ds(g * QCOLS + h * HEAD, HEAD)], dq_recv_sem.at[h, g]).wait()
        here(dk_out.at[:, pl.ds(g * HEAD, HEAD)], dkv_recv_sem.at[0, g]).wait()
        here(dv_out.at[:, pl.ds(g * HEAD, HEAD)], dkv_recv_sem.at[1, g]).wait()
    def wait_sends(copies):
        for copy in copies:
            copy.wait_send()

    wait_sends(sends)
    for h in range(GROUP):
        wait_sends(qe_copies(h))

    for piece in range(PIECES):
        pl.when(has_next)(lambda: wait_sends(halo_copies(1, piece)))
        if piece >= Y:
            pl.when(has_next2)(lambda: wait_sends(halo_copies(2, piece)))
        pl.when(mine != piece)(lambda: wait_sends([dq_copy(h, piece) for h in range(GROUP)] + dkv_copies(piece)))
    for j in range(HALO_BLOCKS):
        pl.when(has_prev if j * BLOCK >= HALF else has_prev2)(lambda: wait_sends(back_copies(j)))


def store(*refs):
    sems = refs[-1]
    copies = [pltpu.make_async_copy(refs[i], refs[i + 3], sems.at[i]) for i in range(3)]
    for copy in copies:
        copy.start()
    for copy in copies:
        copy.wait()


def shards(n_span, query, key, value, out, output_gradient, log_sum_exp, segment_ids):
    hbm = pl.BlockSpec(memory_space=pltpu.HBM)
    dma = pltpu.SemaphoreType.DMA
    shape = jax.ShapeDtypeStruct
    window = HALO + SPAN
    args = (query, key, value, out, output_gradient, log_sum_exp.T, segment_ids.reshape(-1, TOK))
    args = [pltpu.with_memory_space_constraint(a, pltpu.HBM) for a in args]
    grads = pl.pallas_call(
        functools.partial(kernel, n_span),
        out_shape=[
            shape(query.shape, BF16),
            shape(key.shape, BF16),
            shape(value.shape, BF16),
        ],
        in_specs=[hbm] * 7,
        out_specs=[hbm] * 3,
        scratch_shapes=[
            pltpu.VMEM((TOK, PIECES * HEAD), BF16),
            pltpu.VMEM((TOK, PIECES * HEAD), BF16),
            pltpu.VMEM((TOK, PIECES * QCOLS), BF16),
            pltpu.VMEM((TOK, PIECES * QCOLS), BF16),
            pltpu.VMEM((TOK, PIECES * QCOLS), BF16),
            pltpu.VMEM((PIECES * GROUP, TOK), F32),
            pltpu.VMEM((segment_ids.shape[0] // TOK, TOK), jnp.int32),
            pltpu.VMEM((PIECES, 2 * GROUP, TOK), F32),
            pltpu.VMEM((window, HEAD), BF16),
            pltpu.VMEM((window, HEAD), BF16),
            pltpu.VMEM((SPAN, QCOLS), BF16),
            pltpu.VMEM((SPAN, QCOLS), BF16),
            pltpu.VMEM((PIECES, 2 * GROUP, TOK), F32),
            pltpu.VMEM((window, TOK), jnp.int32),
            pltpu.VMEM((1, SPAN), jnp.int32),
            pltpu.VMEM((GROUP, HEAD, SPAN), F32),
            pltpu.VMEM((window, HEAD), F32),
            pltpu.VMEM((window, HEAD), F32),
            pltpu.VMEM((SPAN, QCOLS), BF16),
            pltpu.VMEM((SPAN, HEAD), BF16),
            pltpu.VMEM((SPAN, HEAD), BF16),
            pltpu.VMEM((HALO, HEAD), BF16),
            pltpu.VMEM((HALO, HEAD), BF16),
            pltpu.VMEM((SPAN, HEAD), BF16),
            pltpu.VMEM((SPAN, HEAD), BF16),
            pltpu.VMEM((HALF, HEAD), BF16),
            pltpu.VMEM((HALF, HEAD), BF16),
            dma((7,)),
            dma((2, PIECES)),
            dma((2, PIECES)),
            dma((PIECES,)),
            dma((PIECES,)),
            dma((2, GROUP, PIECES)),
            dma((2, GROUP, PIECES)),
            dma((2, PIECES + Y)),
            dma((2, PIECES + Y)),
            dma((2, HALO_BLOCKS)),
            dma((2, HALO_BLOCKS)),
            dma((GROUP, PIECES)),
            dma((GROUP, PIECES)),
            dma((2, PIECES)),
            dma((2, PIECES)),
        ],
        name="attention_backward",
        compiler_params=pltpu.CompilerParams(
            collective_id=0, has_side_effects=True, vmem_limit_bytes=40 * 2**20
        ),
    )(*args)
    return pl.pallas_call(
        store,
        out_shape=[shape(g.shape, BF16) for g in grads],
        in_specs=[pl.BlockSpec(memory_space=pltpu.VMEM)] * 3,
        out_specs=[hbm] * 3,
        scratch_shapes=[dma((3,))],
        name="store_gradients",
    )(*[pltpu.with_memory_space_constraint(g, pltpu.VMEM) for g in grads])


def solution(mesh):
    rows = P(("seq", "head"), None)
    return jax.shard_map(
        functools.partial(shards, mesh.shape["seq"] // 2),
        mesh=mesh,
        in_specs=(rows,) * 6 + (P(),),
        out_specs=(rows,) * 3,
        check_vma=False,
    )
```
